8 devices in a mesh: dp: 1 (over z), ep: 8 (over y, x, core).
Axes of the slice: x: 2, y: 2, z: 1, core: 2. Of those that a mesh axis runs over, the one named last changes fastest.
Arguments:
- tok_in: bfloat16 [1024, 2048], P(('dp', 'ep'))
- lat_cache: bfloat16 [1024, 128, 512], P(('dp', 'ep'))
- rope_cache: bfloat16 [1024, 128, 64], P(('dp', 'ep'))
- tok_pos: int32 [1024], P(('dp', 'ep'))
- expert_ids: int32 [1024, 6], P(('dp', 'ep'))
- attn_gain: bfloat16 [2048], replicated
- w_query: bfloat16 [2048, 3072], replicated
- w_kvdown: bfloat16 [2048, 576], replicated
- w_ukey: bfloat16 [16, 128, 512], replicated
- w_uval: bfloat16 [16, 512, 128], replicated
- w_out: bfloat16 [2048, 2048], replicated
- ffn_gain: bfloat16 [2048], replicated
- w_router: bfloat16 [2048, 64], replicated
- sh_gate: bfloat16 [2048, 2816], replicated
- sh_up: bfloat16 [2048, 2816], replicated
- sh_down: bfloat16 [2816, 2048], replicated
- ex_gate: bfloat16 [64, 2048, 1408], P('ep')
- ex_up: bfloat16 [64, 2048, 1408], P('ep')
- ex_down: bfloat16 [64, 1408, 2048], P('ep')
Outputs:
- output 1: bfloat16 [1024, 2048], P(('dp', 'ep'))
- output 2: bfloat16 [1024, 128, 512], P(('dp', 'ep'))
- output 3: bfloat16 [1024, 128, 64], P(('dp', 'ep'))
All inputs are finite; a program needn't handle non-finite values.
Results may differ from the reference program's by a relative error of at most 0.0131528.
Values are sent between devices in bfloat16 or wider.
A program may use at most 1 GiB of HBM per device.

```python
import jax
import jax.numpy as jnp
from jax import lax

D_MODEL = 2048
EXP_FF = 1408
NUM_EXPERTS = 64
TOP_K = 6
SHARED_FF = 2816
NUM_HEADS = 16
NOPE_DIM = 128
ROPE_DIM = 64
V_DIM = 128
KV_RANK = 512
TOKENS_DEV = 128
SEQ_LEN = 128
EP_SIZE = 8

NUM_TOKENS = EP_SIZE * TOKENS_DEV
QK_DIM = NOPE_DIM + ROPE_DIM
ATTN_SCALE = QK_DIM ** -0.5
ROUTE_SCALE = 2.827
ROPE_BASE = 10000.0
NORM_EPS = 1e-6


def unit_norm(values):
    mean_sq = jnp.mean(jnp.square(values), axis=-1, keepdims=True)
    return values * lax.rsqrt(mean_sq + NORM_EPS)


def rms_norm(values, gain_vec):
    return unit_norm(values) * gain_vec.astype(jnp.float32)


def rope_rotate(values, angle_rad):
    half_dim = values.shape[-1] // 2
    x_first = values[..., :half_dim]
    x_second = values[..., half_dim:]
    cos_part = jnp.cos(angle_rad)
    sin_part = jnp.sin(angle_rad)
    return jnp.concatenate([x_first * cos_part - x_second * sin_part, x_second * cos_part + x_first * sin_part], axis=-1)


def draw_routing(key):
    cap_slots = max(2, -(-2 * TOKENS_DEV * TOP_K // NUM_EXPERTS))
    pick_total = TOKENS_DEV * TOP_K
    hot_count = pick_total // (2 * cap_slots)
    rest_picks = pick_total - hot_count * cap_slots
    cold_count = NUM_EXPERTS - hot_count
    rank_ids = jnp.arange(NUM_EXPERTS)
    extra_one = ((rank_ids >= hot_count) & (rank_ids < hot_count + rest_picks % cold_count)).astype(jnp.int32)
    count_per = jnp.where(rank_ids < hot_count, cap_slots, rest_picks // cold_count + extra_one)
    slot_ends = jnp.cumsum(count_per)
    slot_rank = jnp.sum((jnp.arange(pick_total)[:, None] >= slot_ends[None, :]).astype(jnp.int32), axis=1)
    rank_table = slot_rank.reshape(TOP_K, TOKENS_DEV).T
    key_perm, key_rows, key_pos, key_high, key_low = jax.random.split(key, 5)
    expert_perm = jax.random.permutation(key_perm, NUM_EXPERTS)
    row_perms = jax.vmap(lambda sub_key: jax.random.permutation(sub_key, TOKENS_DEV))(jax.random.split(key_rows, EP_SIZE))
    rank_rows = rank_table[row_perms]
    expert_ids = expert_perm[rank_rows].reshape(NUM_TOKENS, TOP_K).astype(jnp.int32)
    pos_draw = jax.random.randint(key_pos, (NUM_TOKENS,), SEQ_LEN // 4, SEQ_LEN)
    high_slot = jax.random.randint(key_high, (), 0, NUM_TOKENS)
    low_slot = (high_slot + jax.random.randint(key_low, (), 1, NUM_TOKENS)) % NUM_TOKENS
    tok_ids = jnp.arange(NUM_TOKENS)
    tok_pos = jnp.where(tok_ids == high_slot, SEQ_LEN - 1, jnp.where(tok_ids == low_slot, SEQ_LEN // 4, pos_draw)).astype(jnp.int32)
    return expert_ids, tok_pos


def setup_inputs(seed: int = 0, part: int = 0) -> dict:
    base_key = jax.random.key(seed)
    part_keys = jax.random.split(jax.random.fold_in(base_key, part), 4)
    weight_keys = jax.random.split(base_key, 16)
    expert_ids, tok_pos = draw_routing(jax.random.fold_in(part_keys[0], 1))

    def gain_draw(key, size, center):
        return (center + 0.2 * jax.random.normal(key, (size,), jnp.float32)).astype(jnp.bfloat16)

    def weight_draw(key, shape, fan_in, factor):
        return (jax.random.normal(key, shape, jnp.float32) * factor * fan_in ** -0.5).astype(jnp.bfloat16)

    tok_in = jax.random.normal(part_keys[1], (NUM_TOKENS, D_MODEL), jnp.float32).astype(jnp.bfloat16)
    lat_cache = (1.3 * jax.random.normal(part_keys[2], (NUM_TOKENS, SEQ_LEN, KV_RANK), jnp.float32)).astype(jnp.bfloat16)
    rope_cache = jax.random.normal(part_keys[3], (NUM_TOKENS, SEQ_LEN, ROPE_DIM), jnp.float32).astype(jnp.bfloat16)
    return {
        'tok_in': tok_in,
        'lat_cache': lat_cache,
        'rope_cache': rope_cache,
        'tok_pos': tok_pos,
        'expert_ids': expert_ids,
        'attn_gain': gain_draw(weight_keys[0], D_MODEL, 1.0),
        'w_query': weight_draw(weight_keys[1], (D_MODEL, NUM_HEADS * QK_DIM), D_MODEL, 1.0),
        'w_kvdown': weight_draw(weight_keys[2], (D_MODEL, KV_RANK + ROPE_DIM), D_MODEL, 1.0),
        'w_ukey': weight_draw(weight_keys[4], (NUM_HEADS, NOPE_DIM, KV_RANK), NOPE_DIM, 1.0),
        'w_uval': weight_draw(weight_keys[5], (NUM_HEADS, KV_RANK, V_DIM), KV_RANK, 1.0),
        'w_out': weight_draw(weight_keys[6], (NUM_HEADS * V_DIM, D_MODEL), NUM_HEADS * V_DIM, 1.0),
        'ffn_gain': gain_draw(weight_keys[7], D_MODEL, 1.0),
        'w_router': weight_draw(weight_keys[8], (D_MODEL, NUM_EXPERTS), D_MODEL, 2.0),
        'sh_gate': weight_draw(weight_keys[9], (D_MODEL, SHARED_FF), D_MODEL, 1.0),
        'sh_up': weight_draw(weight_keys[10], (D_MODEL, SHARED_FF), D_MODEL, 1.0),
        'sh_down': weight_draw(weight_keys[11], (SHARED_FF, D_MODEL), SHARED_FF, 1.0),
        'ex_gate': weight_draw(weight_keys[12], (NUM_EXPERTS, D_MODEL, EXP_FF), D_MODEL, 1.0),
        'ex_up': weight_draw(weight_keys[13], (NUM_EXPERTS, D_MODEL, EXP_FF), D_MODEL, 1.0),
        'ex_down': weight_draw(weight_keys[14], (NUM_EXPERTS, EXP_FF, D_MODEL), EXP_FF, 1.0),
    }


def reference(tok_in, lat_cache, rope_cache, tok_pos, expert_ids, attn_gain, w_query, w_kvdown, w_ukey, w_uval, w_out, ffn_gain, w_router, sh_gate, sh_up, sh_down, ex_gate, ex_up, ex_down):
    x_wide = tok_in.astype(jnp.float32)
    x_norm = rms_norm(x_wide, attn_gain).astype(jnp.bfloat16)
    q_all = jnp.dot(x_norm, w_query, preferred_element_type=jnp.float32).astype(jnp.bfloat16).reshape(NUM_TOKENS, NUM_HEADS, QK_DIM)
    kv_all = jnp.dot(x_norm, w_kvdown, preferred_element_type=jnp.float32)
    inv_freq = ROPE_BASE ** (-(2.0 * jnp.arange(ROPE_DIM // 2)) / ROPE_DIM)
    angle_rad = tok_pos.astype(jnp.float32)[:, None] * inv_freq[None, :]
    lat_new = unit_norm(kv_all[:, :KV_RANK]).astype(jnp.bfloat16)
    rope_new = rope_rotate(kv_all[:, KV_RANK:], angle_rad).astype(jnp.bfloat16)
    q_rope = rope_rotate(q_all[:, :, NOPE_DIM:].astype(jnp.float32), angle_rad[:, None, :]).astype(jnp.bfloat16)
    q_lat = jnp.einsum('bhn,hnc->bhc', q_all[:, :, :NOPE_DIM].astype(jnp.float32), w_ukey.astype(jnp.float32)).astype(jnp.bfloat16)
    seq_ids = jnp.arange(SEQ_LEN)
    at_pos = (seq_ids[None, :] == tok_pos[:, None])[:, :, None]
    lat_out = jnp.where(at_pos, lat_new[:, None, :], lat_cache)
    rope_out = jnp.where(at_pos, rope_new[:, None, :], rope_cache)

    def one_token(item_tuple):
        q_lat_t, q_rope_t, lat_t, rope_t, pos_t = item_tuple
        scores = jnp.dot(q_lat_t, lat_t.T, preferred_element_type=jnp.float32)
        scores = scores + jnp.dot(q_rope_t, rope_t.T, preferred_element_type=jnp.float32)
        scores = scores * ATTN_SCALE
        visible = seq_ids[None, :] <= pos_t
        scores = jnp.where(visible, scores, -jnp.inf)
        prob_mat = jax.nn.softmax(scores, axis=-1).astype(jnp.bfloat16)
        return jnp.dot(prob_mat, lat_t, preferred_element_type=jnp.float32).astype(jnp.bfloat16)

    o_lat = lax.map(one_token, (q_lat, q_rope, lat_out, rope_out, tok_pos))
    o_heads = jnp.einsum('bhc,hcv->bhv', o_lat.astype(jnp.float32), w_uval.astype(jnp.float32)).astype(jnp.bfloat16)
    attn_out = jnp.dot(o_heads.reshape(NUM_TOKENS, NUM_HEADS * V_DIM), w_out, preferred_element_type=jnp.float32)
    resid_bf = (x_wide + attn_out).astype(jnp.bfloat16)
    h_norm = rms_norm(resid_bf.astype(jnp.float32), ffn_gain).astype(jnp.bfloat16)
    gate_prob = jax.nn.sigmoid(jnp.dot(h_norm, w_router, preferred_element_type=jnp.float32))
    chosen = jnp.take_along_axis(gate_prob, expert_ids, axis=1)
    route_w = ROUTE_SCALE * chosen / jnp.sum(chosen, axis=1, keepdims=True)
    sh_act = (jax.nn.silu(jnp.dot(h_norm, sh_gate, preferred_element_type=jnp.float32)) * jnp.dot(h_norm, sh_up, preferred_element_type=jnp.float32)).astype(jnp.bfloat16)
    shared_out = jnp.dot(sh_act, sh_down, preferred_element_type=jnp.float32)
    flat_rows = jnp.repeat(h_norm, TOP_K, axis=0)
    flat_ids = expert_ids.reshape(NUM_TOKENS * TOP_K)

    def one_choice(item_tuple):
        row_vec, expert = item_tuple
        row_mat = row_vec[None, :]
        gate_val = jnp.dot(row_mat, ex_gate[expert], preferred_element_type=jnp.float32)
        up_val = jnp.dot(row_mat, ex_up[expert], preferred_element_type=jnp.float32)
        act_val = (jax.nn.silu(gate_val) * up_val).astype(jnp.bfloat16)
        return jnp.dot(act_val, ex_down[expert], preferred_element_type=jnp.float32).astype(jnp.bfloat16)[0]

    choice_out = lax.map(one_choice, (flat_rows, flat_ids)).reshape(NUM_TOKENS, TOP_K, D_MODEL)
    routed = jnp.sum(route_w[:, :, None] * choice_out.astype(jnp.float32), axis=1)
    out_hidden = (resid_bf.astype(jnp.float32) + shared_out + routed).astype(jnp.bfloat16)
    return (out_hidden, lat_out, rope_out)
```

```python
import functools

import jax
import jax.numpy as jnp
from jax import lax
from jax.experimental import pallas as pl
from jax.experimental.pallas import tpu as pltpu
from jax.sharding import PartitionSpec as P

ROUTE_SCALE = 2.827
ROPE_BASE = 10000.0
NORM_EPS = 1e-6
CAP = 24
CHUNK = 256
F32 = jnp.float32
BF16 = jnp.bfloat16


def unit_norm(values):
    mean_sq = jnp.mean(jnp.square(values), axis=-1, keepdims=True)
    return values * lax.rsqrt(mean_sq + NORM_EPS)


def rms_norm(values, gain_vec):
    return unit_norm(values) * gain_vec.astype(jnp.float32)


def rope_rotate(values, angle_rad):
    half_dim = values.shape[-1] // 2
    x_first = values[..., :half_dim]
    x_second = values[..., half_dim:]
    cos_part = jnp.cos(angle_rad)
    sin_part = jnp.sin(angle_rad)
    return jnp.concatenate([x_first * cos_part - x_second * sin_part, x_second * cos_part + x_first * sin_part], axis=-1)


def attention_block(tok_in, lat_cache, rope_cache, tok_pos, attn_gain, w_query, w_kvdown, w_ukey, w_uval, w_out, ffn_gain):
    num_heads, nope_dim, kv_rank = w_ukey.shape
    rope_dim = rope_cache.shape[-1]
    seq_len = lat_cache.shape[1]
    tok_rows = tok_in.shape[0]
    x_wide = tok_in.astype(jnp.float32)
    x_norm = rms_norm(x_wide, attn_gain).astype(jnp.bfloat16)
    q_all = jnp.dot(x_norm, w_query, preferred_element_type=jnp.float32).astype(jnp.bfloat16).reshape(tok_rows, num_heads, nope_dim + rope_dim)
    kv_all = jnp.dot(x_norm, w_kvdown, preferred_element_type=jnp.float32)
    inv_freq = ROPE_BASE ** (-(2.0 * jnp.arange(rope_dim // 2)) / rope_dim)
    angle_rad = tok_pos.astype(jnp.float32)[:, None] * inv_freq[None, :]
    lat_new = unit_norm(kv_all[:, :kv_rank]).astype(jnp.bfloat16)
    rope_new = rope_rotate(kv_all[:, kv_rank:], angle_rad).astype(jnp.bfloat16)
    q_rope = rope_rotate(q_all[:, :, nope_dim:].astype(jnp.float32), angle_rad[:, None, :]).astype(jnp.bfloat16)
    q_lat = jnp.einsum('bhn,hnc->bhc', q_all[:, :, :nope_dim], w_ukey, preferred_element_type=jnp.float32).astype(jnp.bfloat16)
    seq_ids = jnp.arange(seq_len)
    at_pos = (seq_ids[None, :] == tok_pos[:, None])[:, :, None]
    lat_out = jnp.where(at_pos, lat_new[:, None, :], lat_cache)
    rope_out = jnp.where(at_pos, rope_new[:, None, :], rope_cache)
    scores = jnp.einsum('bhc,bsc->bhs', q_lat, lat_out, preferred_element_type=jnp.float32)
    scores = scores + jnp.einsum('bhr,bsr->bhs', q_rope, rope_out, preferred_element_type=jnp.float32)
    scores = scores * (nope_dim + rope_dim) ** -0.5
    visible = (seq_ids[None, :] <= tok_pos[:, None])[:, None, :]
    scores = jnp.where(visible, scores, -jnp.inf)
    prob_mat = jax.nn.softmax(scores, axis=-1).astype(jnp.bfloat16)
    o_lat = jnp.einsum('bhs,bsc->bhc', prob_mat, lat_out, preferred_element_type=jnp.float32).astype(jnp.bfloat16)
    o_heads = jnp.einsum('bhc,hcv->bhv', o_lat, w_uval, preferred_element_type=jnp.float32).astype(jnp.bfloat16)
    attn_out = jnp.dot(o_heads.reshape(tok_rows, -1), w_out, preferred_element_type=jnp.float32)
    resid_bf = (x_wide + attn_out).astype(jnp.bfloat16)
    h_norm = rms_norm(resid_bf.astype(jnp.float32), ffn_gain).astype(jnp.bfloat16)
    return resid_bf, h_norm, lat_out, rope_out


def route_table(h_norm, w_router, expert_ids):
    num_experts = w_router.shape[1]
    gate_prob = jax.nn.sigmoid(jnp.dot(h_norm, w_router, preferred_element_type=jnp.float32))
    picked = jnp.any(expert_ids[:, :, None] == jnp.arange(num_experts)[None, None, :], axis=1)
    chosen = jnp.where(picked, gate_prob, 0.0)
    table = ROUTE_SCALE * chosen / jnp.sum(chosen, axis=1, keepdims=True)
    return table.T


def moe_kernel(h_ref, rw_ref, res_ref, eg, eu, ed, sg, su, sd, out_ref,
               ring, hall, xbuf, actt, actsh, acc, drecv, r1, r2, stage, base, pw, pwf, pbuf, ebuf, rwin,
               ring_sem, ag_s, ag_r, rw_s, rw_r, d_s, d_r, s1_s, s1_r, s2_s, s2_r):
    rows = h_ref.shape[0]
    half = rows // 2
    d_model = h_ref.shape[1]
    ff = eg.shape[2]
    n_exp = eg.shape[0]
    n_chunk = d_model // CHUNK
    grp = 2 * CAP
    mids = [(n, min(CHUNK, ff - n)) for n in range(0, ff, CHUNK)]
    me = lax.axis_index('ep')
    core = me % 2
    cx = (me // 2) % 2
    cy = me // 4
    mate = me + 1 - 2 * core
    xn = me + 2 - 4 * cx
    yn = me + 4 - 8 * cy
    dg = yn + 2 - 4 * cx
    others = [(0, 1, mate), (1, 0, xn), (1, 1, xn + 1 - 2 * core), (2, 0, yn), (2, 1, yn + 1 - 2 * core), (3, 0, dg), (3, 1, dg + 1 - 2 * core)]

    def remote(src, dst, ssem, rsem, dev):
        return pltpu.make_async_remote_copy(src_ref=src, dst_ref=dst, send_sem=ssem, recv_sem=rsem, device_id={'ep': dev}, device_id_type=pl.DeviceIdType.MESH)

    step = d_model // 4

    def pair_copies(slot, gate, up):
        out = []
        for b, src in enumerate((gate, up)):
            for q in range(4):
                out.append(pltpu.make_async_copy(src.at[pl.ds(q * step, step), :], ring.at[slot, b, pl.ds(q * step, step), :], ring_sem.at[slot, b * 4 + q]))
        return out

    def shared_copies(slot, i):
        return pair_copies(slot, sg.at[:, pl.ds(i * ff, ff)], su.at[:, pl.ds(i * ff, ff)])

    def expert_copies(slot, e):
        return pair_copies(slot, eg.at[e], eu.at[e])

    def tile_at(slot, i):
        return ring.at[slot, i // 5, pl.ds(0, ff), pl.ds((i % 5) * CHUNK, CHUNK)]

    def down_copies(slot, j):
        cols = pl.ds(pl.multiple_of(j * CHUNK, CHUNK), CHUNK)
        out = [pltpu.make_async_copy(ed.at[e, :, cols], tile_at(slot, e), ring_sem.at[slot, e]) for e in range(n_exp)]
        for i in range(2):
            out.append(pltpu.make_async_copy(sd.at[pl.ds(i * ff, ff), cols], tile_at(slot, n_exp + i), ring_sem.at[slot, n_exp + i]))
        return out

    def start(copies):
        for c in copies:
            c.start()

    def wait(copies):
        for c in copies:
            c.wait()

    start(shared_copies(0, 0))
    start(shared_copies(1, 1))
    start(expert_copies(2, 0))

    barrier = pltpu.get_barrier_semaphore()
    for _, _, dev in others:
        pl.semaphore_signal(barrier, inc=1, device_id={'ep': dev}, device_id_type=pl.DeviceIdType.MESH)
    pl.semaphore_wait(barrier, len(others))

    part_a, part_b = pl.ds(0, half), pl.ds(half, half)
    own, other = pl.ds(0, rows), pl.ds(rows, rows)
    rw_copies = [remote(rw_ref.at[pl.ds(pl.multiple_of(dev * n_exp, n_exp), n_exp), :], rwin.at[r, p], rw_s.at[i], rw_r.at[i], dev) for i, (r, p, dev) in enumerate(others)]
    start(rw_copies)
    to_mate = remote(h_ref, hall.at[0, other], ag_s.at[0], ag_r.at[0], mate)
    x_a = remote(h_ref.at[part_a], hall.at[1, part_a], ag_s.at[1], ag_r.at[1], xn)
    x_b = remote(h_ref.at[part_b], hall.at[1, part_b], ag_s.at[2], ag_r.at[2], xn)
    y_b = remote(h_ref.at[part_b], hall.at[2, part_b], ag_s.at[3], ag_r.at[3], yn)
    y_a = remote(h_ref.at[part_a], hall.at[2, part_a], ag_s.at[4], ag_r.at[4], yn)
    d_a = remote(hall.at[1, part_a], hall.at[3, part_a], ag_s.at[5], ag_r.at[5], yn)
    d_b = remote(hall.at[2, part_b], hall.at[3, part_b], ag_s.at[6], ag_r.at[6], xn)
    m_x = remote(hall.at[1, own], hall.at[1, other], ag_s.at[7], ag_r.at[7], mate)
    m_y = remote(hall.at[2, own], hall.at[2, other], ag_s.at[8], ag_r.at[8], mate)
    m_d = remote(hall.at[3, own], hall.at[3, other], ag_s.at[9], ag_r.at[9], mate)
    for c in (x_a, y_b, to_mate, x_b, y_a):
        c.start()

    hall[0, 0:rows, :] = h_ref[...]
    rwin[0, 0] = rw_ref[pl.ds(pl.multiple_of(me * n_exp, n_exp), n_exp), :]
    for c in rw_copies:
        c.wait_recv()

    def gather_rows(r):
        both = jnp.concatenate([rwin[r, 0], rwin[r, 1]], axis=1)
        two = 2 * rows
        t_in = lax.broadcasted_iota(jnp.int32, (two, two), 0)
        t_out = lax.broadcasted_iota(jnp.int32, (two, two), 1)
        ahead = jnp.where((t_in < t_out) & ((t_in < rows) == (t_out < rows)), 1.0, 0.0).astype(BF16)
        picked = both > 0.0
        before = jnp.dot(jnp.where(picked, 1.0, 0.0).astype(BF16), ahead, preferred_element_type=F32)
        lane = lax.broadcasted_iota(jnp.int32, (n_exp, two), 1)
        slot = jnp.where(picked, before + jnp.where(lane < rows, 0.0, float(CAP)), -1.0).astype(jnp.int32)
        want = lax.broadcasted_iota(jnp.int32, (grp, two), 0)
        for e in range(n_exp):
            hit = want == slot[e:e + 1, :]
            pbuf[e * grp:(e + 1) * grp, :] = jnp.where(hit, 1.0, 0.0).astype(BF16)
            pwf[e * grp:(e + 1) * grp, :] = jnp.where(hit, both[e:e + 1, :], 0.0)
        wide = 512
        for n in range(0, d_model, wide):
            got = jnp.dot(pbuf[...], hall[r, :, n:n + wide], preferred_element_type=F32).astype(BF16)
            for e in range(n_exp):
                xbuf[e, r * grp:(r + 1) * grp, n:n + wide] = got[e * grp:(e + 1) * grp, :]
        turned = pwf[...].T
        hi = turned.astype(BF16)
        rest = turned - hi.astype(F32)
        mid = rest.astype(BF16)
        pw[r, 0] = hi
        pw[r, 1] = mid
        pw[r, 2] = (rest - mid.astype(F32)).astype(BF16)

    def shared_item(i):
        wait(shared_copies(i, i))
        for n, w in mids:
            g = jnp.dot(h_ref[...], ring[i, 0, :, n:n + w], preferred_element_type=F32)
            u = jnp.dot(h_ref[...], ring[i, 1, :, n:n + w], preferred_element_type=F32)
            actsh[i, :, n:n + w] = (jax.nn.silu(g) * u).astype(BF16)
        start(expert_copies(i, i + 1))

    shared_item(0)
    x_a.wait_recv()
    d_a.start()
    y_b.wait_recv()
    d_b.start()
    to_mate.wait_recv()
    gather_rows(0)
    shared_item(1)
    x_b.wait_recv()
    m_x.start()
    y_a.wait_recv()
    m_y.start()
    m_x.wait_recv()
    gather_rows(1)
    m_y.wait_recv()
    gather_rows(2)
    d_a.wait_recv()
    d_b.wait_recv()
    m_d.start()
    m_d.wait_recv()
    gather_rows(3)

    @pl.loop(0, n_exp)
    def _(e):
        slot = (e + 2) % 3
        wait(expert_copies(slot, e))
        for n, w in mids:
            g = jnp.dot(xbuf[e], ring[slot, 0, :, n:n + w], preferred_element_type=F32)
            u = jnp.dot(xbuf[e], ring[slot, 1, :, n:n + w], preferred_element_type=F32)
            actt[:, n:n + w] = (jax.nn.silu(g) * u).astype(BF16)
        xbuf[e, :, 0:ff] = actt[...]

        @pl.when(e + 3 < n_exp)
        def _():
            start(expert_copies(slot, e + 3))

        @pl.when(e + 3 >= n_exp)
        def _():
            start(down_copies(slot, e + 3 - n_exp))

    def first_stage(j):
        odd = j % 2
        dev = xn + odd * (yn - xn)
        return [remote(acc.at[j, 1 + odd], r1.at[j, 0], s1_s.at[j, 0], s1_r.at[j, 0], dev), remote(acc.at[j, 3], r1.at[j, 1], s1_s.at[j, 1], s1_r.at[j, 1], dev)]

    def second_stage(j):
        odd = j % 2
        dev = yn + odd * (xn - yn)
        return remote(acc.at[j, 2 - odd], r2.at[j], s2_s.at[j], s2_r.at[j], dev)

    def swap(j):
        return remote(stage.at[j % 2], drecv.at[j], d_s.at[j], d_r.at[j], mate)

    def send_sum(j):
        swap(j).wait_recv()
        acc[j] = acc[j] + drecv[j]
        start(first_stage(j))

    @pl.loop(0, n_chunk)
    def _(j):
        slot = (j + n_exp + 2) % 3
        wait(down_copies(slot, j))
        for e in range(n_exp):
            tile = ring[slot, e // 5, 0:ff, (e % 5) * CHUNK:(e % 5 + 1) * CHUNK]
            got = jnp.dot(xbuf[e, :, 0:ff], tile, preferred_element_type=F32).astype(BF16)
            for r in range(4):
                ebuf[r, e * grp:(e + 1) * grp, :] = got[r * grp:(r + 1) * grp, :]

        @pl.when(j >= 2)
        def _():
            swap(j - 2).wait_send()

        for r in range(4):
            part = jnp.dot(pw[r, 0], ebuf[r], preferred_element_type=F32)
            part = part + jnp.dot(pw[r, 1], ebuf[r], preferred_element_type=F32)
            part = part + jnp.dot(pw[r, 2], ebuf[r], preferred_element_type=F32)
            acc[j, r] = part[0:rows, :]
            stage[j % 2, r] = part[rows:, :]
        swap(j).start()

        cols = pl.ds(pl.multiple_of(j * CHUNK, CHUNK), CHUNK)
        total = res_ref[:, cols].astype(F32)
        for i in range(2):
            k = n_exp + i
            tile = ring[slot, k // 5, 0:ff, (k % 5) * CHUNK:(k % 5 + 1) * CHUNK]
            total = total + jnp.dot(actsh[i], tile, preferred_element_type=F32)
        base[j] = total

        @pl.when(j + 3 < n_chunk)
        def _():
            start(down_copies(slot, j + 3))

        @pl.when(j >= 1)
        def _():
            send_sum(j - 1)

    send_sum(n_chunk - 1)

    @pl.loop(0, n_chunk)
    def _(j):
        for c in first_stage(j):
            c.wait_recv()
        passed = 2 - j % 2
        acc[j, passed] = acc[j, passed] + r1[j, 1]
        second_stage(j).start()
        base[j] = base[j] + (acc[j, 0] + r1[j, 0])

    @pl.loop(0, n_chunk)
    def _(j):
        second_stage(j).wait_recv()
        cols = pl.ds(pl.multiple_of(j * CHUNK, CHUNK), CHUNK)
        out_ref[:, cols] = (base[j] + r2[j]).astype(BF16)

    for c in rw_copies + [to_mate, x_a, x_b, y_a, y_b, d_a, d_b, m_x, m_y, m_d]:
        c.wait_send()
    swap(n_chunk - 2).wait_send()
    swap(n_chunk - 1).wait_send()

    @pl.loop(0, n_chunk)
    def _(j):
        for c in first_stage(j):
            c.wait_send()
        second_stage(j).wait_send()


def moe(h, table, resid, eg, eu, ed, sg, su, sd):
    rows, d_model = h.shape
    n_exp, _, ff = eg.shape
    n_chunk = d_model // CHUNK
    slots = 8 * CAP
    vmem = pl.BlockSpec(memory_space=pltpu.VMEM)
    hbm = pl.BlockSpec(memory_space=pl.ANY)
    dma = pltpu.SemaphoreType.DMA
    scratch = [
        pltpu.VMEM((3, 2, d_model, ff), BF16),
        pltpu.VMEM((4, 2 * rows, d_model), BF16),
        pltpu.VMEM((n_exp, slots, d_model), BF16),
        pltpu.VMEM((slots, ff), BF16),
        pltpu.VMEM((2, rows, ff), BF16),
        pltpu.VMEM((n_chunk, 4, rows, CHUNK), F32),
        pltpu.VMEM((n_chunk, 4, rows, CHUNK), F32),
        pltpu.VMEM((n_chunk, 2, rows, CHUNK), F32),
        pltpu.VMEM((n_chunk, rows, CHUNK), F32),
        pltpu.VMEM((2, 4, rows, CHUNK), F32),
        pltpu.VMEM((n_chunk, rows, CHUNK), F32),
        pltpu.VMEM((4, 3, 2 * rows, n_exp * 2 * CAP), BF16),
        pltpu.VMEM((n_exp * 2 * CAP, 2 * rows), F32),
        pltpu.VMEM((n_exp * 2 * CAP, 2 * rows), BF16),
        pltpu.VMEM((4, n_exp * 2 * CAP, CHUNK), BF16),
        pltpu.VMEM((4, 2, n_exp, rows), F32),
        dma((3, 10)), dma((10,)), dma((10,)), dma((7,)), dma((7,)), dma((n_chunk,)), dma((n_chunk,)),
        dma((n_chunk, 2)), dma((n_chunk, 2)), dma((n_chunk,)), dma((n_chunk,)),
    ]
    return pl.pallas_call(
        moe_kernel,
        out_shape=jax.ShapeDtypeStruct((rows, d_model), BF16),
        in_specs=[vmem] * 3 + [hbm] * 6,
        out_specs=vmem,
        scratch_shapes=scratch,
        compiler_params=pltpu.CompilerParams(collective_id=0, has_side_effects=True, vmem_limit_bytes=67043328),
        cost_estimate=pl.CostEstimate(flops=40_000_000_000, bytes_accessed=175_000_000, transcendentals=0),
    )(h, table, resid, eg, eu, ed, sg, su, sd)


def solution(mesh):
    row_one = P(('dp', 'ep'))
    row_two = P(('dp', 'ep'), None)
    row_three = P(('dp', 'ep'), None, None)
    rep_one = P(None)
    rep_two = P(None, None)
    rep_three = P(None, None, None)
    exp_spec = P('ep', None, None)

    def local_step(tok_in, lat_cache, rope_cache, tok_pos, expert_ids, attn_gain, w_query, w_kvdown, w_ukey, w_uval, w_out, ffn_gain, w_router, sh_gate, sh_up, sh_down, ex_gate, ex_up, ex_down):
        resid_bf, h_norm, lat_out, rope_out = attention_block(tok_in, lat_cache, rope_cache, tok_pos, attn_gain, w_query, w_kvdown, w_ukey, w_uval, w_out, ffn_gain)
        table = route_table(h_norm, w_router, expert_ids)
        out_hidden = moe(h_norm, table, resid_bf, ex_gate, ex_up, ex_down, sh_gate, sh_up, sh_down)
        return out_hidden, lat_out, rope_out

    in_specs = (row_two, row_three, row_three, row_one, row_two, rep_one, rep_two, rep_two, rep_three, rep_three, rep_two, rep_one, rep_two, rep_two, rep_two, rep_two, exp_spec, exp_spec, exp_spec)
    out_specs = (row_two, row_three, row_three)
    return jax.shard_map(local_step, mesh=mesh, in_specs=in_specs, out_specs=out_specs, check_vma=False)
```

```python
import jax
import jax.numpy as jnp
from jax import lax
from jax.experimental import pallas as pl
from jax.experimental.pallas import tpu as pltpu
from jax.sharding import PartitionSpec as P

ROUTE_SCALE = 2.827
ROPE_BASE = 10000.0
NORM_EPS = 1e-6
CAP = 24
CHUNK = 256
BLK = 16
F32 = jnp.float32
BF16 = jnp.bfloat16


def attn_kernel(pos_ref, x_ref, gain_ref, cos_ref, sin_ref, ids_ref, fgain_ref, wkv, wq, wuk, wuv, wo, wr, lat_in, rope_in,
                lat_out, rope_out, res_ref, h_ref, rw_ref,
                vkv, vq, vuk, vuv, vo, vr, lat, rop, xn, qlat, qrope, latn, ropen, olat, ohd, w_sem, lat_sem, rope_sem, lo_sem, ro_sem):
    rows, d_model = x_ref.shape
    n_head, nope, rank = wuk.shape
    rdim = rope_in.shape[1]
    seq = lat_in.shape[1]
    qk = nope + rdim
    n_blk = rows // BLK
    scale = qk ** -0.5
    pair = 2 * qk
    n_pair = n_head // 2

    def q_copy(m):
        cols = slice(m * pair, (m + 1) * pair)
        return pltpu.make_async_copy(wq.at[:, cols], vq.at[:, cols], w_sem.at[m])

    kv_copy = pltpu.make_async_copy(wkv, vkv, w_sem.at[n_pair])
    uk_copy = pltpu.make_async_copy(wuk, vuk, w_sem.at[n_pair + 1])
    uv_copy = pltpu.make_async_copy(wuv, vuv, w_sem.at[n_pair + 2])
    o_copy = pltpu.make_async_copy(wo, vo, w_sem.at[n_pair + 3])
    r_copy = pltpu.make_async_copy(wr, vr, w_sem.at[n_pair + 4])

    def lat_load(b):
        return pltpu.make_async_copy(lat_in.at[pl.ds(b * BLK, BLK)], lat.at[pl.ds(b * BLK, BLK)], lat_sem.at[b])

    def rope_load(b):
        return pltpu.make_async_copy(rope_in.at[pl.ds(b * BLK, BLK)], rop.at[pl.ds(b * BLK, BLK)], rope_sem.at[b])

    def lat_save(b):
        return pltpu.make_async_copy(lat.at[pl.ds(b * BLK, BLK)], lat_out.at[pl.ds(b * BLK, BLK)], lo_sem.at[b])

    def rope_save(b):
        return pltpu.make_async_copy(rop.at[pl.ds(b * BLK, BLK)], rope_out.at[pl.ds(b * BLK, BLK)], ro_sem.at[b])

    kv_copy.start()
    for m in range(n_pair):
        q_copy(m).start()
        if m == 0:
            uk_copy.start()

    @pl.loop(0, n_blk)
    def _(b):
        lat_load(b).start()
        rope_load(b).start()

    uv_copy.start()
    o_copy.start()
    r_copy.start()

    xw = x_ref[...].astype(F32)
    xn[...] = (xw * lax.rsqrt(jnp.mean(xw * xw, axis=-1, keepdims=True) + NORM_EPS) * gain_ref[...].astype(F32)).astype(BF16)
    lane = lax.broadcasted_iota(jnp.int32, (rows, 2 * rdim), 1)
    front = lane % rdim < rdim // 2
    low = lane < rdim
    cos_t = cos_ref[...]
    sin_t = sin_ref[...]

    def rotate(v):
        swapped = jnp.where(front, pltpu.roll(v, 2 * rdim - rdim // 2, 1), pltpu.roll(v, rdim // 2, 1))
        return v * cos_t + swapped * sin_t

    kv_copy.wait()
    kv = lax.dot_general(xn[...], vkv[...], (((1,), (1,)), ((), ())), preferred_element_type=F32)
    lat_raw = kv[:, 0:rank]
    latn[...] = (lat_raw * lax.rsqrt(jnp.mean(lat_raw * lat_raw, axis=-1, keepdims=True) + NORM_EPS)).astype(BF16).astype(F32)
    kr = kv[:, rank:rank + rdim]
    ropen[...] = rotate(jnp.concatenate([kr, kr], axis=1)).astype(BF16).astype(F32)

    for m in range(n_pair):
        q_copy(m).wait()
        if m == 0:
            uk_copy.wait()
        qf = jnp.dot(xn[...], vq[:, m * pair:(m + 1) * pair], preferred_element_type=F32).astype(BF16).astype(F32)
        qa, qb, qc = qf[:, 0:nope], qf[:, nope:2 * nope], qf[:, 2 * nope:3 * nope]
        second = pltpu.roll(jnp.where(low, qc, qb), rdim, 1)
        turned = rotate(jnp.where(low, qb, qc))
        qrope[2 * m] = turned[:, 0:rdim].astype(BF16)
        qrope[2 * m + 1] = pltpu.roll(turned, rdim, 1)[:, 0:rdim].astype(BF16)
        qlat[2 * m] = jnp.dot(qa.astype(BF16), vuk[2 * m], preferred_element_type=F32).astype(BF16)
        qlat[2 * m + 1] = jnp.dot(second.astype(BF16), vuk[2 * m + 1], preferred_element_type=F32).astype(BF16)

    grp = BLK * n_head
    row_i = lax.broadcasted_iota(jnp.int32, (grp, grp), 0)
    col_i = lax.broadcasted_iota(jnp.int32, (grp, grp), 1)
    perm = jnp.where(col_i == (row_i % n_head) * BLK + row_i // n_head, 1.0, 0.0).astype(BF16)

    @pl.loop(0, n_blk)
    def _(b):
        t0 = pl.multiple_of(b * BLK, BLK)
        lat_load(b).wait()
        rope_load(b).wait()
        news = jnp.transpose(ropen[pl.ds(t0, BLK), :])
        slane = lax.broadcasted_iota(jnp.int32, (rdim, seq), 1)
        srow = lax.broadcasted_iota(jnp.int32, (16, rank), 0)
        for t in range(BLK):
            p = pos_ref[t0 + t]
            lo = pl.multiple_of((p // 16) * 16, 16)
            old = lat[t0 + t, pl.ds(lo, 16), :]
            lat[t0 + t, pl.ds(lo, 16), :] = jnp.where(srow == p - lo, latn[pl.ds(t0 + t, 1), :], old.astype(F32)).astype(BF16)
            rop[t0 + t] = jnp.where(slane == p, news[0:rdim, t:t + 1], rop[t0 + t].astype(F32)).astype(BF16)
        q_blk = jnp.dot(perm, qlat[:, pl.ds(t0, BLK), :].reshape(grp, rank), preferred_element_type=F32).astype(BF16)
        r_blk = jnp.dot(perm, qrope[:, pl.ds(t0, BLK), :].reshape(grp, rdim), preferred_element_type=F32).astype(BF16)
        klane = lax.broadcasted_iota(jnp.int32, (n_head, seq), 1)
        scores = []
        for t in range(BLK):
            s = lax.dot_general(q_blk[t * n_head:(t + 1) * n_head], lat[t0 + t], (((1,), (1,)), ((), ())), preferred_element_type=F32)
            s = s + jnp.dot(r_blk[t * n_head:(t + 1) * n_head], rop[t0 + t], preferred_element_type=F32)
            scores.append(jnp.where(klane <= pos_ref[t0 + t], s * scale, -jnp.inf))
        sc = jnp.concatenate(scores, axis=0)
        ex = jnp.exp(sc - jnp.max(sc, axis=-1, keepdims=True))
        prob = (ex / jnp.sum(ex, axis=-1, keepdims=True)).astype(BF16)
        outs = [jnp.dot(prob[t * n_head:(t + 1) * n_head], lat[t0 + t], preferred_element_type=F32).astype(BF16) for t in range(BLK)]
        mixed = jnp.dot(perm, jnp.concatenate(outs, axis=0), preferred_element_type=F32).astype(BF16)
        olat[:, pl.ds(t0, BLK), :] = mixed.reshape(n_head, BLK, rank)
        lat_save(b).start()
        rope_save(b).start()

    uv_copy.wait()
    for h in range(n_head):
        ohd[:, h * nope:(h + 1) * nope] = jnp.dot(olat[h], vuv[h], preferred_element_type=F32).astype(BF16)
    o_copy.wait()
    total = jnp.zeros((rows, 1), F32)
    wide = 512
    for n in range(0, d_model, wide):
        part = jnp.dot(ohd[...], vo[:, n:n + wide], preferred_element_type=F32)
        res = (x_ref[:, n:n + wide].astype(F32) + part).astype(BF16)
        res_ref[:, n:n + wide] = res
        resf = res.astype(F32)
        total = total + jnp.sum(resf * resf, axis=-1, keepdims=True)
    inv = lax.rsqrt(total * (1.0 / d_model) + NORM_EPS)
    for n in range(0, d_model, wide):
        h_ref[:, n:n + wide] = (res_ref[:, n:n + wide].astype(F32) * inv * fgain_ref[:, n:n + wide].astype(F32)).astype(BF16)
    r_copy.wait()
    gate = jax.nn.sigmoid(lax.dot_general(vr[...], h_ref[...], (((1,), (1,)), ((), ())), preferred_element_type=F32))
    want = lax.broadcasted_iota(jnp.int32, gate.shape, 0)
    picked = want == ids_ref[0:1, :]
    for k in range(1, ids_ref.shape[0]):
        picked = picked | (want == ids_ref[k:k + 1, :])
    chosen = jnp.where(picked, gate, 0.0)
    rw_ref[...] = ROUTE_SCALE * chosen / jnp.sum(chosen, axis=0, keepdims=True)

    @pl.loop(0, n_blk)
    def _(b):
        lat_save(b).wait()
        rope_save(b).wait()


def attention(tok_in, lat_cache, rope_cache, tok_pos, expert_ids, attn_gain, w_query, w_kvdown, w_ukey, w_uval, w_out, ffn_gain, w_router):
    rows, d_model = tok_in.shape
    n_head, nope, rank = w_ukey.shape
    seq, rdim = rope_cache.shape[1], rope_cache.shape[2]
    n_exp = w_router.shape[1]
    inv_freq = ROPE_BASE ** (-(2.0 * jnp.arange(rdim // 2)) / rdim)
    angle = tok_pos.astype(F32)[:, None] * jnp.tile(inv_freq, 4)[None, :]
    sign = jnp.tile(jnp.where(jnp.arange(rdim) < rdim // 2, -1.0, 1.0), 2)[None, :]
    vmem = pl.BlockSpec(memory_space=pltpu.VMEM)
    smem = pl.BlockSpec(memory_space=pltpu.SMEM)
    hbm = pl.BlockSpec(memory_space=pl.ANY)
    dma = pltpu.SemaphoreType.DMA
    n_blk = rows // BLK
    scratch = [
        pltpu.VMEM((rank + rdim, d_model), BF16),
        pltpu.VMEM(w_query.shape, BF16),
        pltpu.VMEM(w_ukey.shape, BF16),
        pltpu.VMEM(w_uval.shape, BF16),
        pltpu.VMEM(w_out.shape, BF16),
        pltpu.VMEM((n_exp, d_model), BF16),
        pltpu.VMEM(lat_cache.shape, BF16),
        pltpu.VMEM((rows, rdim, seq), BF16),
        pltpu.VMEM((rows, d_model), BF16),
        pltpu.VMEM((n_head, rows, rank), BF16),
        pltpu.VMEM((n_head, rows, rdim), BF16),
        pltpu.VMEM((rows, rank), F32),
        pltpu.VMEM((rows, 2 * rdim), F32),
        pltpu.VMEM((n_head, rows, rank), BF16),
        pltpu.VMEM((rows, n_head * nope), BF16),
        dma((n_head // 2 + 5,)), dma((n_blk,)), dma((n_blk,)), dma((n_blk,)), dma((n_blk,)),
    ]
    lat_out, rope_out, resid, h, table = pl.pallas_call(
        attn_kernel,
        out_shape=(
            jax.ShapeDtypeStruct(lat_cache.shape, BF16),
            jax.ShapeDtypeStruct((rows, rdim, seq), BF16),
            jax.ShapeDtypeStruct((rows, d_model), BF16),
            jax.ShapeDtypeStruct((rows, d_model), BF16),
            jax.ShapeDtypeStruct((n_exp, rows), F32),
        ),
        in_specs=[smem] + [vmem] * 6 + [hbm] * 8,
        out_specs=(hbm, hbm, vmem, vmem, vmem),
        scratch_shapes=scratch,
        compiler_params=pltpu.CompilerParams(vmem_limit_bytes=64000000),
        cost_estimate=pl.CostEstimate(flops=5_000_000_000, bytes_accessed=66_000_000, transcendentals=0),
    )(tok_pos, tok_in, attn_gain[None, :], jnp.cos(angle), jnp.sin(angle) * sign, expert_ids.T, ffn_gain[None, :],
      w_kvdown.T, w_query, w_ukey, w_uval, w_out, w_router.T, lat_cache, jnp.swapaxes(rope_cache, 1, 2))
    return resid, h, table, lat_out, jnp.swapaxes(rope_out, 1, 2)


def moe_kernel(h_ref, rw_ref, res_ref, eg, eu, ed, sg, su, sd, out_ref,
               ring, hall, xbuf, actt, actsh, acc, drecv, r1, r2, stage, base, pw, pwf, pbuf, ebuf, rwin,
               ring_sem, ag_s, ag_r, rw_s, rw_r, d_s, d_r, s1_s, s1_r, s2_s, s2_r):
    rows = h_ref.shape[0]
    half = rows // 2
    d_model = h_ref.shape[1]
    ff = eg.shape[2]
    n_exp = eg.shape[0]
    n_chunk = d_model // CHUNK
    grp = 2 * CAP
    mids = [(n, min(CHUNK, ff - n)) for n in range(0, ff, CHUNK)]
    me = lax.axis_index('ep')
    core = me % 2
    cx = (me // 2) % 2
    cy = me // 4
    mate = me + 1 - 2 * core
    xn = me + 2 - 4 * cx
    yn = me + 4 - 8 * cy
    dg = yn + 2 - 4 * cx
    others = [(0, 1, mate), (1, 0, xn), (1, 1, xn + 1 - 2 * core), (2, 0, yn), (2, 1, yn + 1 - 2 * core), (3, 0, dg), (3, 1, dg + 1 - 2 * core)]

    def remote(src, dst, ssem, rsem, dev):
        return pltpu.make_async_remote_copy(src_ref=src, dst_ref=dst, send_sem=ssem, recv_sem=rsem, device_id={'ep': dev}, device_id_type=pl.DeviceIdType.MESH)

    step = d_model // 4

    def pair_copies(slot, gate, up):
        out = []
        for b, src in enumerate((gate, up)):
            for q in range(4):
                out.append(pltpu.make_async_copy(src.at[pl.ds(q * step, step), :], ring.at[slot, b, pl.ds(q * step, step), :], ring_sem.at[slot, b * 4 + q]))
        return out

    def shared_copies(slot, i):
        return pair_copies(slot, sg.at[:, pl.ds(i * ff, ff)], su.at[:, pl.ds(i * ff, ff)])

    def expert_copies(slot, e):
        return pair_copies(slot, eg.at[e], eu.at[e])

    def tile_at(slot, i):
        return ring.at[slot, i // 5, pl.ds(0, ff), pl.ds((i % 5) * CHUNK, CHUNK)]

    def down_copies(slot, j):
        cols = pl.ds(pl.multiple_of(j * CHUNK, CHUNK), CHUNK)
        out = [pltpu.make_async_copy(ed.at[e, :, cols], tile_at(slot, e), ring_sem.at[slot, e]) for e in range(n_exp)]
        for i in range(2):
            out.append(pltpu.make_async_copy(sd.at[pl.ds(i * ff, ff), cols], tile_at(slot, n_exp + i), ring_sem.at[slot, n_exp + i]))
        return out

    def start(copies):
        for c in copies:
            c.start()

    def wait(copies):
        for c in copies:
            c.wait()

    start(shared_copies(0, 0))
    start(shared_copies(1, 1))
    start(expert_copies(2, 0))

    barrier = pltpu.get_barrier_semaphore()
    for _, _, dev in others:
        pl.semaphore_signal(barrier, inc=1, device_id={'ep': dev}, device_id_type=pl.DeviceIdType.MESH)
    pl.semaphore_wait(barrier, len(others))

    part_a, part_b = pl.ds(0, half), pl.ds(half, half)
    own, other = pl.ds(0, rows), pl.ds(rows, rows)
    rw_copies = [remote(rw_ref.at[pl.ds(pl.multiple_of(dev * n_exp, n_exp), n_exp), :], rwin.at[r, p], rw_s.at[i], rw_r.at[i], dev) for i, (r, p, dev) in enumerate(others)]
    start(rw_copies)
    to_mate = remote(h_ref, hall.at[0, other], ag_s.at[0], ag_r.at[0], mate)
    x_a = remote(h_ref.at[part_a], hall.at[1, part_a], ag_s.at[1], ag_r.at[1], xn)
    x_b = remote(h_ref.at[part_b], hall.at[1, part_b], ag_s.at[2], ag_r.at[2], xn)
    y_b = remote(h_ref.at[part_b], hall.at[2, part_b], ag_s.at[3], ag_r.at[3], yn)
    y_a = remote(h_ref.at[part_a], hall.at[2, part_a], ag_s.at[4], ag_r.at[4], yn)
    d_a = remote(hall.at[1, part_a], hall.at[3, part_a], ag_s.at[5], ag_r.at[5], yn)
    d_b = remote(hall.at[2, part_b], hall.at[3, part_b], ag_s.at[6], ag_r.at[6], xn)
    m_x = remote(hall.at[1, own], hall.at[1, other], ag_s.at[7], ag_r.at[7], mate)
    m_y = remote(hall.at[2, own], hall.at[2, other], ag_s.at[8], ag_r.at[8], mate)
    m_d = remote(hall.at[3, own], hall.at[3, other], ag_s.at[9], ag_r.at[9], mate)
    for c in (x_a, y_b, to_mate, x_b, y_a):
        c.start()

    hall[0, 0:rows, :] = h_ref[...]
    rwin[0, 0] = rw_ref[pl.ds(pl.multiple_of(me * n_exp, n_exp), n_exp), :]
    for c in rw_copies:
        c.wait_recv()

    def gather_rows(r):
        both = jnp.concatenate([rwin[r, 0], rwin[r, 1]], axis=1)
        two = 2 * rows
        t_in = lax.broadcasted_iota(jnp.int32, (two, two), 0)
        t_out = lax.broadcasted_iota(jnp.int32, (two, two), 1)
        ahead = jnp.where((t_in < t_out) & ((t_in < rows) == (t_out < rows)), 1.0, 0.0).astype(BF16)
        picked = both > 0.0
        before = jnp.dot(jnp.where(picked, 1.0, 0.0).astype(BF16), ahead, preferred_element_type=F32)
        lane = lax.broadcasted_iota(jnp.int32, (n_exp, two), 1)
        slot = jnp.where(picked, before + jnp.where(lane < rows, 0.0, float(CAP)), -1.0).astype(jnp.int32)
        want = lax.broadcasted_iota(jnp.int32, (grp, two), 0)
        for e in range(n_exp):
            hit = want == slot[e:e + 1, :]
            pbuf[e * grp:(e + 1) * grp, :] = jnp.where(hit, 1.0, 0.0).astype(BF16)
            pwf[e * grp:(e + 1) * grp, :] = jnp.where(hit, both[e:e + 1, :], 0.0)
        wide = 512
        for n in range(0, d_model, wide):
            got = jnp.dot(pbuf[...], hall[r, :, n:n + wide], preferred_element_type=F32).astype(BF16)
            for e in range(n_exp):
                xbuf[e, r * grp:(r + 1) * grp, n:n + wide] = got[e * grp:(e + 1) * grp, :]
        turned = pwf[...].T
        hi = turned.astype(BF16)
        rest = turned - hi.astype(F32)
        mid = rest.astype(BF16)
        pw[r, 0] = hi
        pw[r, 1] = mid
        pw[r, 2] = (rest - mid.astype(F32)).astype(BF16)

    def shared_item(i):
        wait(shared_copies(i, i))
        for n, w in mids:
            g = jnp.dot(h_ref[...], ring[i, 0, :, n:n + w], preferred_element_type=F32)
            u = jnp.dot(h_ref[...], ring[i, 1, :, n:n + w], preferred_element_type=F32)
            actsh[i, :, n:n + w] = (jax.nn.silu(g) * u).astype(BF16)
        start(expert_copies(i, i + 1))

    shared_item(0)
    x_a.wait_recv()
    d_a.start()
    y_b.wait_recv()
    d_b.start()
    to_mate.wait_recv()
    gather_rows(0)
    shared_item(1)
    x_b.wait_recv()
    m_x.start()
    y_a.wait_recv()
    m_y.start()
    m_x.wait_recv()
    gather_rows(1)
    m_y.wait_recv()
    gather_rows(2)
    d_a.wait_recv()
    d_b.wait_recv()
    m_d.start()
    m_d.wait_recv()
    gather_rows(3)

    @pl.loop(0, n_exp)
    def _(e):
        slot = (e + 2) % 3
        wait(expert_copies(slot, e))
        for n, w in mids:
            g = jnp.dot(xbuf[e], ring[slot, 0, :, n:n + w], preferred_element_type=F32)
            u = jnp.dot(xbuf[e], ring[slot, 1, :, n:n + w], preferred_element_type=F32)
            actt[:, n:n + w] = (jax.nn.silu(g) * u).astype(BF16)
        xbuf[e, :, 0:ff] = actt[...]

        @pl.when(e + 3 < n_exp)
        def _():
            start(expert_copies(slot, e + 3))

        @pl.when(e + 3 >= n_exp)
        def _():
            start(down_copies(slot, e + 3 - n_exp))

    def first_stage(j):
        odd = j % 2
        dev = xn + odd * (yn - xn)
        return [remote(acc.at[j, 1 + odd], r1.at[j, 0], s1_s.at[j, 0], s1_r.at[j, 0], dev), remote(acc.at[j, 3], r1.at[j, 1], s1_s.at[j, 1], s1_r.at[j, 1], dev)]

    def second_stage(j):
        odd = j % 2
        dev = yn + odd * (xn - yn)
        return remote(acc.at[j, 2 - odd], r2.at[j], s2_s.at[j], s2_r.at[j], dev)

    def swap(j):
        return remote(stage.at[j % 2], drecv.at[j], d_s.at[j], d_r.at[j], mate)

    def send_sum(j):
        swap(j).wait_recv()
        acc[j] = acc[j] + drecv[j]
        start(first_stage(j))

    @pl.loop(0, n_chunk)
    def _(j):
        slot = (j + n_exp + 2) % 3
        wait(down_copies(slot, j))
        for e in range(n_exp):
            tile = ring[slot, e // 5, 0:ff, (e % 5) * CHUNK:(e % 5 + 1) * CHUNK]
            got = jnp.dot(xbuf[e, :, 0:ff], tile, preferred_element_type=F32).astype(BF16)
            for r in range(4):
                ebuf[r, e * grp:(e + 1) * grp, :] = got[r * grp:(r + 1) * grp, :]

        @pl.when(j >= 2)
        def _():
            swap(j - 2).wait_send()

        for r in range(4):
            part = jnp.dot(pw[r, 0], ebuf[r], preferred_element_type=F32)
            part = part + jnp.dot(pw[r, 1], ebuf[r], preferred_element_type=F32)
            part = part + jnp.dot(pw[r, 2], ebuf[r], preferred_element_type=F32)
            acc[j, r] = part[0:rows, :]
            stage[j % 2, r] = part[rows:, :]
        swap(j).start()

        cols = pl.ds(pl.multiple_of(j * CHUNK, CHUNK), CHUNK)
        total = res_ref[:, cols].astype(F32)
        for i in range(2):
            k = n_exp + i
            tile = ring[slot, k // 5, 0:ff, (k % 5) * CHUNK:(k % 5 + 1) * CHUNK]
            total = total + jnp.dot(actsh[i], tile, preferred_element_type=F32)
        base[j] = total

        @pl.when(j + 3 < n_chunk)
        def _():
            start(down_copies(slot, j + 3))

        @pl.when(j >= 1)
        def _():
            send_sum(j - 1)

    send_sum(n_chunk - 1)

    @pl.loop(0, n_chunk)
    def _(j):
        for c in first_stage(j):
            c.wait_recv()
        passed = 2 - j % 2
        acc[j, passed] = acc[j, passed] + r1[j, 1]
        second_stage(j).start()
        base[j] = base[j] + (acc[j, 0] + r1[j, 0])

    @pl.loop(0, n_chunk)
    def _(j):
        second_stage(j).wait_recv()
        cols = pl.ds(pl.multiple_of(j * CHUNK, CHUNK), CHUNK)
        out_ref[:, cols] = (base[j] + r2[j]).astype(BF16)

    for c in rw_copies + [to_mate, x_a, x_b, y_a, y_b, d_a, d_b, m_x, m_y, m_d]:
        c.wait_send()
    swap(n_chunk - 2).wait_send()
    swap(n_chunk - 1).wait_send()

    @pl.loop(0, n_chunk)
    def _(j):
        for c in first_stage(j):
            c.wait_send()
        second_stage(j).wait_send()


def moe(h, table, resid, eg, eu, ed, sg, su, sd):
    rows, d_model = h.shape
    n_exp, _, ff = eg.shape
    n_chunk = d_model // CHUNK
    slots = 8 * CAP
    vmem = pl.BlockSpec(memory_space=pltpu.VMEM)
    hbm = pl.BlockSpec(memory_space=pl.ANY)
    dma = pltpu.SemaphoreType.DMA
    scratch = [
        pltpu.VMEM((3, 2, d_model, ff), BF16),
        pltpu.VMEM((4, 2 * rows, d_model), BF16),
        pltpu.VMEM((n_exp, slots, d_model), BF16),
        pltpu.VMEM((slots, ff), BF16),
        pltpu.VMEM((2, rows, ff), BF16),
        pltpu.VMEM((n_chunk, 4, rows, CHUNK), F32),
        pltpu.VMEM((n_chunk, 4, rows, CHUNK), F32),
        pltpu.VMEM((n_chunk, 2, rows, CHUNK), F32),
        pltpu.VMEM((n_chunk, rows, CHUNK), F32),
        pltpu.VMEM((2, 4, rows, CHUNK), F32),
        pltpu.VMEM((n_chunk, rows, CHUNK), F32),
        pltpu.VMEM((4, 3, 2 * rows, n_exp * 2 * CAP), BF16),
        pltpu.VMEM((n_exp * 2 * CAP, 2 * rows), F32),
        pltpu.VMEM((n_exp * 2 * CAP, 2 * rows), BF16),
        pltpu.VMEM((4, n_exp * 2 * CAP, CHUNK), BF16),
        pltpu.VMEM((4, 2, n_exp, rows), F32),
        dma((3, 10)), dma((10,)), dma((10,)), dma((7,)), dma((7,)), dma((n_chunk,)), dma((n_chunk,)),
        dma((n_chunk, 2)), dma((n_chunk, 2)), dma((n_chunk,)), dma((n_chunk,)),
    ]
    return pl.pallas_call(
        moe_kernel,
        out_shape=jax.ShapeDtypeStruct((rows, d_model), BF16),
        in_specs=[vmem] * 3 + [hbm] * 6,
        out_specs=vmem,
        scratch_shapes=scratch,
        compiler_params=pltpu.CompilerParams(collective_id=0, has_side_effects=True, vmem_limit_bytes=67043328),
        cost_estimate=pl.CostEstimate(flops=40_000_000_000, bytes_accessed=175_000_000, transcendentals=0),
    )(h, table, resid, eg, eu, ed, sg, su, sd)


def solution(mesh):
    row_one = P(('dp', 'ep'))
    row_two = P(('dp', 'ep'), None)
    row_three = P(('dp', 'ep'), None, None)
    rep_one = P(None)
    rep_two = P(None, None)
    rep_three = P(None, None, None)
    exp_spec = P('ep', None, None)

    def local_step(tok_in, lat_cache, rope_cache, tok_pos, expert_ids, attn_gain, w_query, w_kvdown, w_ukey, w_uval, w_out, ffn_gain, w_router, sh_gate, sh_up, sh_down, ex_gate, ex_up, ex_down):
        resid_bf, h_norm, table, lat_out, rope_out = attention(tok_in, lat_cache, rope_cache, tok_pos, expert_ids, attn_gain, w_query, w_kvdown, w_ukey, w_uval, w_out, ffn_gain, w_router)
        out_hidden = moe(h_norm, table, resid_bf, ex_gate, ex_up, ex_down, sh_gate, sh_up, sh_down)
        return out_hidden, lat_out, rope_out

    in_specs = (row_two, row_three, row_three, row_one, row_two, rep_one, rep_two, rep_two, rep_three, rep_three, rep_two, rep_one, rep_two, rep_two, rep_two, rep_two, exp_spec, exp_spec, exp_spec)
    out_specs = (row_two, row_three, row_three)
    return jax.shard_map(local_step, mesh=mesh, in_specs=in_specs, out_specs=out_specs, check_vma=False)
```

```python
import jax
import jax.numpy as jnp
import numpy as np
from jax import lax
from jax.experimental import pallas as pl
from jax.experimental.pallas import tpu as pltpu
from jax.sharding import PartitionSpec as P

ROUTE_SCALE = 2.827
ROPE_BASE = 10000.0
NORM_EPS = 1e-6
CAP = 24
CHUNK = 256
BLK = 16
LAG = 4
F32 = jnp.float32
BF16 = jnp.bfloat16


def attn_kernel(pos_ref, prow_ref, x_ref, gain_ref, ids_ref, fgain_ref, wkv, wq, wuk, wuv, wo, wr, lat_in, rope_in,
                lat_out, rope_out, res_ref, h_ref, rw_ref,
                vkv, vq, vuk, vuv, vo, vr, lat, rop, xn, qlat, qrope, latn, ropen, olat, ohd, w_sem, lat_sem, rope_sem, lo_sem, ro_sem):
    rows, d_model = x_ref.shape
    n_head, nope, rank = wuk.shape
    rdim = rope_in.shape[1]
    seq = lat_in.shape[1]
    qk = nope + rdim
    n_blk = rows // BLK
    scale = qk ** -0.5
    pair = 2 * qk
    n_pair = n_head // 2

    def q_copy(m):
        cols = slice(m * pair, (m + 1) * pair)
        return pltpu.make_async_copy(wq.at[:, cols], vq.at[:, cols], w_sem.at[m])

    kv_copy = pltpu.make_async_copy(wkv, vkv, w_sem.at[n_pair])
    uk_copy = pltpu.make_async_copy(wuk, vuk, w_sem.at[n_pair + 1])
    uv_copy = pltpu.make_async_copy(wuv, vuv, w_sem.at[n_pair + 2])
    o_copy = pltpu.make_async_copy(wo, vo, w_sem.at[n_pair + 3])
    r_copy = pltpu.make_async_copy(wr, vr, w_sem.at[n_pair + 4])

    def lat_load(b):
        return pltpu.make_async_copy(lat_in.at[pl.ds(b * BLK, BLK)], lat.at[pl.ds(b * BLK, BLK)], lat_sem.at[b])

    def rope_load(b):
        return pltpu.make_async_copy(rope_in.at[pl.ds(b * BLK, BLK)], rop.at[pl.ds(b * BLK, BLK)], rope_sem.at[b])

    def lat_save(b):
        return pltpu.make_async_copy(lat.at[pl.ds(b * BLK, BLK)], lat_out.at[pl.ds(b * BLK, BLK)], lo_sem.at[b])

    def rope_save(b):
        return pltpu.make_async_copy(rop.at[pl.ds(b * BLK, BLK)], rope_out.at[pl.ds(b * BLK, BLK)], ro_sem.at[b])

    kv_copy.start()
    for m in range(n_pair):
        q_copy(m).start()
        if m == 0:
            uk_copy.start()

    @pl.loop(0, n_blk)
    def _(b):
        lat_load(b).start()
        rope_load(b).start()

    uv_copy.start()
    o_copy.start()
    r_copy.start()

    xw = x_ref[...].astype(F32)
    xn[...] = (xw * lax.rsqrt(jnp.mean(xw * xw, axis=-1, keepdims=True) + NORM_EPS) * gain_ref[...].reshape(1, d_model).astype(F32)).astype(BF16)
    lane = lax.broadcasted_iota(jnp.int32, (rows, 2 * rdim), 1)
    front = lane % rdim < rdim // 2
    low = lane < rdim
    where_in = lane % (rdim // 2)
    freq = jnp.zeros(lane.shape, F32)
    for i in range(rdim // 2):
        freq = jnp.where(where_in == i, np.float32(ROPE_BASE ** (-2.0 * i / rdim)), freq)
    angle = jnp.transpose(jnp.broadcast_to(prow_ref[...].astype(F32), (rows, rows))) * freq
    cos_t = jnp.cos(angle)
    sin_t = jnp.where(front, -jnp.sin(angle), jnp.sin(angle))

    def rotate(v):
        swapped = jnp.where(front, pltpu.roll(v, 2 * rdim - rdim // 2, 1), pltpu.roll(v, rdim // 2, 1))
        return v * cos_t + swapped * sin_t

    kv_copy.wait()
    kv = lax.dot_general(xn[...], vkv[...], (((1,), (1,)), ((), ())), preferred_element_type=F32)
    lat_raw = kv[:, 0:rank]
    latn[...] = (lat_raw * lax.rsqrt(jnp.mean(lat_raw * lat_raw, axis=-1, keepdims=True) + NORM_EPS)).astype(BF16).astype(F32)
    kr = kv[:, rank:rank + rdim]
    ropen[...] = rotate(jnp.concatenate([kr, kr], axis=1)).astype(BF16).astype(F32)

    for m in range(n_pair):
        q_copy(m).wait()
        if m == 0:
            uk_copy.wait()
        qf = jnp.dot(xn[...], vq[:, m * pair:(m + 1) * pair], preferred_element_type=F32).astype(BF16).astype(F32)
        qa, qb, qc = qf[:, 0:nope], qf[:, nope:2 * nope], qf[:, 2 * nope:3 * nope]
        second = pltpu.roll(jnp.where(low, qc, qb), rdim, 1)
        turned = rotate(jnp.where(low, qb, qc))
        qrope[2 * m] = turned[:, 0:rdim].astype(BF16)
        qrope[2 * m + 1] = pltpu.roll(turned, rdim, 1)[:, 0:rdim].astype(BF16)
        qlat[2 * m] = jnp.dot(qa.astype(BF16), vuk[2 * m], preferred_element_type=F32).astype(BF16)
        qlat[2 * m + 1] = jnp.dot(second.astype(BF16), vuk[2 * m + 1], preferred_element_type=F32).astype(BF16)

    grp = BLK * n_head
    row_i = lax.broadcasted_iota(jnp.int32, (grp, grp), 0)
    col_i = lax.broadcasted_iota(jnp.int32, (grp, grp), 1)
    perm = jnp.where(col_i == (row_i % n_head) * BLK + row_i // n_head, 1.0, 0.0).astype(BF16)

    @pl.loop(0, n_blk)
    def _(b):
        t0 = pl.multiple_of(b * BLK, BLK)
        lat_load(b).wait()
        rope_load(b).wait()
        news = jnp.transpose(ropen[pl.ds(t0, BLK), :])
        slane = lax.broadcasted_iota(jnp.int32, (rdim, seq), 1)
        srow = lax.broadcasted_iota(jnp.int32, (16, rank), 0)
        for t in range(BLK):
            p = pos_ref[t0 + t]
            lo = pl.multiple_of((p // 16) * 16, 16)
            old = lat[t0 + t, pl.ds(lo, 16), :]
            lat[t0 + t, pl.ds(lo, 16), :] = jnp.where(srow == p - lo, latn[pl.ds(t0 + t, 1), :], old.astype(F32)).astype(BF16)
            rop[t0 + t] = jnp.where(slane == p, news[0:rdim, t:t + 1], rop[t0 + t].astype(F32)).astype(BF16)
        q_blk = jnp.dot(perm, qlat[:, pl.ds(t0, BLK), :].reshape(grp, rank), preferred_element_type=F32).astype(BF16)
        r_blk = jnp.dot(perm, qrope[:, pl.ds(t0, BLK), :].reshape(grp, rdim), preferred_element_type=F32).astype(BF16)
        klane = lax.broadcasted_iota(jnp.int32, (n_head, seq), 1)
        scores = []
        for t in range(BLK):
            s = lax.dot_general(q_blk[t * n_head:(t + 1) * n_head], lat[t0 + t], (((1,), (1,)), ((), ())), preferred_element_type=F32)
            s = s + jnp.dot(r_blk[t * n_head:(t + 1) * n_head], rop[t0 + t], preferred_element_type=F32)
            scores.append(jnp.where(klane <= pos_ref[t0 + t], s * scale, -jnp.inf))
        sc = jnp.concatenate(scores, axis=0)
        ex = jnp.exp(sc - jnp.max(sc, axis=-1, keepdims=True))
        prob = (ex / jnp.sum(ex, axis=-1, keepdims=True)).astype(BF16)
        outs = [jnp.dot(prob[t * n_head:(t + 1) * n_head], lat[t0 + t], preferred_element_type=F32).astype(BF16) for t in range(BLK)]
        mixed = jnp.dot(perm, jnp.concatenate(outs, axis=0), preferred_element_type=F32).astype(BF16)
        olat[:, pl.ds(t0, BLK), :] = mixed.reshape(n_head, BLK, rank)
        lat_save(b).start()
        rope_save(b).start()

    uv_copy.wait()
    for h in range(n_head):
        ohd[:, h * nope:(h + 1) * nope] = jnp.dot(olat[h], vuv[h], preferred_element_type=F32).astype(BF16)
    o_copy.wait()
    total = jnp.zeros((rows, 1), F32)
    wide = 512
    for n in range(0, d_model, wide):
        part = jnp.dot(ohd[...], vo[:, n:n + wide], preferred_element_type=F32)
        res = (x_ref[:, n:n + wide].astype(F32) + part).astype(BF16)
        res_ref[:, n:n + wide] = res
        resf = res.astype(F32)
        total = total + jnp.sum(resf * resf, axis=-1, keepdims=True)
    fgain = fgain_ref[...].reshape(1, d_model).astype(F32)
    inv = lax.rsqrt(total * (1.0 / d_model) + NORM_EPS)
    for n in range(0, d_model, wide):
        h_ref[:, n:n + wide] = (res_ref[:, n:n + wide].astype(F32) * inv * fgain[:, n:n + wide]).astype(BF16)
    r_copy.wait()
    gate = jax.nn.sigmoid(lax.dot_general(vr[...], h_ref[...], (((1,), (1,)), ((), ())), preferred_element_type=F32))
    want = lax.broadcasted_iota(jnp.int32, gate.shape, 0)
    picked = want == ids_ref[0:1, :]
    for k in range(1, ids_ref.shape[0]):
        picked = picked | (want == ids_ref[k:k + 1, :])
    chosen = jnp.where(picked, gate, 0.0)
    rw_ref[...] = ROUTE_SCALE * chosen / jnp.sum(chosen, axis=0, keepdims=True)

    @pl.loop(0, n_blk)
    def _(b):
        lat_save(b).wait()
        rope_save(b).wait()


def attention(tok_in, lat_cache, rope_cache, tok_pos, expert_ids, attn_gain, w_query, w_kvdown, w_ukey, w_uval, w_out, ffn_gain, w_router):
    rows, d_model = tok_in.shape
    n_head, nope, rank = w_ukey.shape
    seq, rdim = rope_cache.shape[1], rope_cache.shape[2]
    n_exp = w_router.shape[1]
    vmem = pl.BlockSpec(memory_space=pltpu.VMEM)
    smem = pl.BlockSpec(memory_space=pltpu.SMEM)
    hbm = pl.BlockSpec(memory_space=pl.ANY)
    dma = pltpu.SemaphoreType.DMA
    n_blk = rows // BLK
    scratch = [
        pltpu.VMEM((rank + rdim, d_model), BF16),
        pltpu.VMEM(w_query.shape, BF16),
        pltpu.VMEM(w_ukey.shape, BF16),
        pltpu.VMEM(w_uval.shape, BF16),
        pltpu.VMEM(w_out.shape, BF16),
        pltpu.VMEM((n_exp, d_model), BF16),
        pltpu.VMEM(lat_cache.shape, BF16),
        pltpu.VMEM((rows, rdim, seq), BF16),
        pltpu.VMEM((rows, d_model), BF16),
        pltpu.VMEM((n_head, rows, rank), BF16),
        pltpu.VMEM((n_head, rows, rdim), BF16),
        pltpu.VMEM((rows, rank), F32),
        pltpu.VMEM((rows, 2 * rdim), F32),
        pltpu.VMEM((n_head, rows, rank), BF16),
        pltpu.VMEM((rows, n_head * nope), BF16),
        dma((n_head // 2 + 5,)), dma((n_blk,)), dma((n_blk,)), dma((n_blk,)), dma((n_blk,)),
    ]
    lat_out, rope_out, resid, h, table = pl.pallas_call(
        attn_kernel,
        out_shape=(
            jax.ShapeDtypeStruct(lat_cache.shape, BF16),
            jax.ShapeDtypeStruct((rows, rdim, seq), BF16),
            jax.ShapeDtypeStruct((rows, d_model), BF16),
            jax.ShapeDtypeStruct((rows, d_model), BF16),
            jax.ShapeDtypeStruct((n_exp, rows), F32),
        ),
        in_specs=[smem] + [vmem] * 5 + [hbm] * 8,
        out_specs=(hbm, hbm, vmem, vmem, vmem),
        scratch_shapes=scratch,
        compiler_params=pltpu.CompilerParams(vmem_limit_bytes=64000000),
        cost_estimate=pl.CostEstimate(flops=5_000_000_000, bytes_accessed=66_000_000, transcendentals=0),
    )(tok_pos, tok_pos[None, :], tok_in, attn_gain, expert_ids.T, ffn_gain,
      w_kvdown.T, w_query, w_ukey, w_uval, w_out, w_router.T, lat_cache, jnp.swapaxes(rope_cache, 1, 2))
    return resid, h, table, lat_out, jnp.swapaxes(rope_out, 1, 2)


def moe_kernel(h_ref, rw_ref, res_hbm, eg, eu, ed, sg, su, sd, out_ref,
               ring, hall, xbuf, actt, actsh, acc, drecv, r1, r2, stage, base, pw, pwf, pbuf, ebuf, rwin,
               ring_sem, res_sem, ag_s, ag_r, rw_s, rw_r, d_s, d_r, s1_s, s1_r, s2_s, s2_r):
    rows = h_ref.shape[0]
    half = rows // 2
    d_model = h_ref.shape[1]
    ff = eg.shape[2]
    n_exp = eg.shape[0]
    n_chunk = d_model // CHUNK
    grp = 2 * CAP
    mids = [(n, min(CHUNK, ff - n)) for n in range(0, ff, CHUNK)]
    me = lax.axis_index('ep')
    core = me % 2
    cx = (me // 2) % 2
    cy = me // 4
    mate = me + 1 - 2 * core
    xn = me + 2 - 4 * cx
    yn = me + 4 - 8 * cy
    dg = yn + 2 - 4 * cx
    others = [(0, 1, mate), (1, 0, xn), (1, 1, xn + 1 - 2 * core), (2, 0, yn), (2, 1, yn + 1 - 2 * core), (3, 0, dg), (3, 1, dg + 1 - 2 * core)]

    def remote(src, dst, ssem, rsem, dev):
        return pltpu.make_async_remote_copy(src_ref=src, dst_ref=dst, send_sem=ssem, recv_sem=rsem, device_id={'ep': dev}, device_id_type=pl.DeviceIdType.MESH)

    step = d_model // 4

    def pair_copies(slot, gate, up):
        out = []
        for b, src in enumerate((gate, up)):
            for q in range(4):
                out.append(pltpu.make_async_copy(src.at[pl.ds(q * step, step), :], ring.at[slot, b, pl.ds(q * step, step), :], ring_sem.at[slot, b * 4 + q]))
        return out

    def shared_copies(slot, i):
        return pair_copies(slot, sg.at[:, pl.ds(i * ff, ff)], su.at[:, pl.ds(i * ff, ff)])

    def expert_copies(slot, e):
        return pair_copies(slot, eg.at[e], eu.at[e])

    def tile_at(slot, i):
        return ring.at[slot, i // 5, pl.ds(0, ff), pl.ds((i % 5) * CHUNK, CHUNK)]

    def down_copies(slot, j):
        cols = pl.ds(pl.multiple_of(j * CHUNK, CHUNK), CHUNK)
        out = [pltpu.make_async_copy(ed.at[e, :, cols], tile_at(slot, e), ring_sem.at[slot, e]) for e in range(n_exp)]
        for i in range(2):
            out.append(pltpu.make_async_copy(sd.at[pl.ds(i * ff, ff), cols], tile_at(slot, n_exp + i), ring_sem.at[slot, n_exp + i]))
        return out

    def start(copies):
        for c in copies:
            c.start()

    def wait(copies):
        for c in copies:
            c.wait()

    barrier = pltpu.get_barrier_semaphore()
    for _, _, dev in others:
        pl.semaphore_signal(barrier, inc=1, device_id={'ep': dev}, device_id_type=pl.DeviceIdType.MESH)
    start(shared_copies(0, 0))
    start(shared_copies(1, 1))
    start(expert_copies(2, 0))
    res_copy = pltpu.make_async_copy(res_hbm, out_ref, res_sem)
    res_copy.start()
    pl.semaphore_wait(barrier, len(others))

    part_a, part_b = pl.ds(0, half), pl.ds(half, half)
    own, other = pl.ds(0, rows), pl.ds(rows, rows)
    rw_copies = [remote(rw_ref.at[pl.ds(pl.multiple_of(dev * n_exp, n_exp), n_exp), :], rwin.at[r, p], rw_s.at[i], rw_r.at[i], dev) for i, (r, p, dev) in enumerate(others)]
    start(rw_copies)
    to_mate = remote(h_ref, hall.at[0, other], ag_s.at[0], ag_r.at[0], mate)
    x_a = remote(h_ref.at[part_a], hall.at[1, part_a], ag_s.at[1], ag_r.at[1], xn)
    x_b = remote(h_ref.at[part_b], hall.at[1, part_b], ag_s.at[2], ag_r.at[2], xn)
    y_b = remote(h_ref.at[part_b], hall.at[2, part_b], ag_s.at[3], ag_r.at[3], yn)
    y_a = remote(h_ref.at[part_a], hall.at[2, part_a], ag_s.at[4], ag_r.at[4], yn)
    d_a = remote(hall.at[1, part_a], hall.at[3, part_a], ag_s.at[5], ag_r.at[5], yn)
    d_b = remote(hall.at[2, part_b], hall.at[3, part_b], ag_s.at[6], ag_r.at[6], xn)
    m_x = remote(hall.at[1, own], hall.at[1, other], ag_s.at[7], ag_r.at[7], mate)
    m_y = remote(hall.at[2, own], hall.at[2, other], ag_s.at[8], ag_r.at[8], mate)
    m_da = remote(hall.at[3, part_a], hall.at[3, pl.ds(rows, half)], ag_s.at[9], ag_r.at[9], mate)
    m_db = remote(hall.at[3, part_b], hall.at[3, pl.ds(rows + half, half)], ag_s.at[10], ag_r.at[10], mate)
    for c in (x_a, y_b, to_mate, x_b, y_a):
        c.start()

    hall[0, 0:rows, :] = h_ref[...]
    rwin[0, 0] = rw_ref[pl.ds(pl.multiple_of(me * n_exp, n_exp), n_exp), :]
    for c in rw_copies:
        c.wait_recv()

    def tables(r):
        both = jnp.concatenate([rwin[r, 0], rwin[r, 1]], axis=1)
        two = 2 * rows
        t_in = lax.broadcasted_iota(jnp.int32, (two, two), 0)
        t_out = lax.broadcasted_iota(jnp.int32, (two, two), 1)
        ahead = jnp.where((t_in < t_out) & ((t_in < rows) == (t_out < rows)), 1.0, 0.0).astype(BF16)
        picked = both > 0.0
        before = jnp.dot(jnp.where(picked, 1.0, 0.0).astype(BF16), ahead, preferred_element_type=F32)
        lane = lax.broadcasted_iota(jnp.int32, (n_exp, two), 1)
        slot = jnp.where(picked, before + jnp.where(lane < rows, 0.0, float(CAP)), -1.0).astype(jnp.int32)
        want = lax.broadcasted_iota(jnp.int32, (grp, two), 0)
        for e in range(n_exp):
            hit = want == slot[e:e + 1, :]
            pbuf[r, e * grp:(e + 1) * grp, :] = jnp.where(hit, 1.0, 0.0).astype(BF16)
            pwf[e * grp:(e + 1) * grp, :] = jnp.where(hit, both[e:e + 1, :], 0.0)
        turned = pwf[...].T
        hi = turned.astype(BF16)
        rest = turned - hi.astype(F32)
        mid = rest.astype(BF16)
        pw[r, 0] = hi
        pw[r, 1] = mid
        pw[r, 2] = (rest - mid.astype(F32)).astype(BF16)

    def gather_rows(r):
        wide = 512
        for n in range(0, d_model, wide):
            got = jnp.dot(pbuf[r], hall[r, :, n:n + wide], preferred_element_type=F32).astype(BF16)
            for e in range(n_exp):
                xbuf[e, r * grp:(r + 1) * grp, n:n + wide] = got[e * grp:(e + 1) * grp, :]

    def shared_item(i):
        wait(shared_copies(i, i))
        for n, w in mids:
            g = jnp.dot(h_ref[...], ring[i, 0, :, n:n + w], preferred_element_type=F32)
            u = jnp.dot(h_ref[...], ring[i, 1, :, n:n + w], preferred_element_type=F32)
            actsh[i, :, n:n + w] = (jax.nn.silu(g) * u).astype(BF16)
        start(expert_copies(i, i + 1))

    for r in range(4):
        tables(r)
    to_mate.wait_recv()
    gather_rows(0)
    shared_item(0)
    x_a.wait_recv()
    d_a.start()
    y_b.wait_recv()
    d_b.start()
    shared_item(1)
    x_b.wait_recv()
    m_x.start()
    y_a.wait_recv()
    m_y.start()
    m_x.wait_recv()
    gather_rows(1)
    m_y.wait_recv()
    gather_rows(2)
    d_a.wait_recv()
    m_da.start()
    d_b.wait_recv()
    m_db.start()
    m_da.wait_recv()
    m_db.wait_recv()
    gather_rows(3)
    res_copy.wait()

    @pl.loop(0, n_exp)
    def _(e):
        slot = (e + 2) % 3
        wait(expert_copies(slot, e))
        for n, w in mids:
            g = jnp.dot(xbuf[e], ring[slot, 0, :, n:n + w], preferred_element_type=F32)
            u = jnp.dot(xbuf[e], ring[slot, 1, :, n:n + w], preferred_element_type=F32)
            actt[:, n:n + w] = (jax.nn.silu(g) * u).astype(BF16)
        xbuf[e, :, 0:ff] = actt[...]

        @pl.when(e + 3 < n_exp)
        def _():
            start(expert_copies(slot, e + 3))

        @pl.when(e + 3 >= n_exp)
        def _():
            start(down_copies(slot, e + 3 - n_exp))

    side = CHUNK // 2

    def first_stage(j):
        out = []
        for f, dev in enumerate((xn, yn)):
            for q, r in enumerate((1 + f, 3)):
                out.append(remote(acc.at[j, f, r], r1.at[j, f, q], s1_s.at[j, 2 * f + q], s1_r.at[j, 2 * f + q], dev))
        return out

    def second_stage(j):
        return [remote(acc.at[j, f, 2 - f], r2.at[j, f], s2_s.at[j, f], s2_r.at[j, f], dev) for f, dev in enumerate((yn, xn))]

    def swap(j):
        return remote(stage.at[j % 2], drecv.at[j], d_s.at[j], d_r.at[j], mate)

    def send_sum(j):
        swap(j).wait_recv()
        acc[j] = acc[j] + drecv[j]
        start(first_stage(j))

    def pass_on(j):
        for c in first_stage(j):
            c.wait_recv()
        for f, c in enumerate(second_stage(j)):
            acc[j, f, 2 - f] = acc[j, f, 2 - f] + r1[j, f, 1]
            c.start()
        for f in range(2):
            cut = slice(f * side, (f + 1) * side)
            base[j, :, cut] = base[j, :, cut] + (acc[j, f, 0] + r1[j, f, 0])

    @pl.loop(0, n_chunk)
    def _(j):
        slot = (j + n_exp + 2) % 3
        wait(down_copies(slot, j))
        for e in range(n_exp):
            if e == n_exp // 2:
                pl.when(j >= 2)(lambda: send_sum(j - 1))
            tile = ring[slot, e // 5, 0:ff, (e % 5) * CHUNK:(e % 5 + 1) * CHUNK]
            got = jnp.dot(xbuf[e, :, 0:ff], tile, preferred_element_type=F32).astype(BF16)
            for r in range(4):
                ebuf[r, e * grp:(e + 1) * grp, :] = got[r * grp:(r + 1) * grp, :]

        @pl.when(j >= 2)
        def _():
            swap(j - 2).wait_send()

        for r in range(4):
            part = jnp.dot(pw[r, 0], ebuf[r], preferred_element_type=F32)
            part = part + jnp.dot(pw[r, 1], ebuf[r], preferred_element_type=F32)
            part = part + jnp.dot(pw[r, 2], ebuf[r], preferred_element_type=F32)
            for f in range(2):
                cut = slice(f * side, (f + 1) * side)
                acc[j, f, r] = part[0:rows, cut]
                stage[j % 2, f, r] = part[rows:, cut]
        swap(j).start()

        cols = pl.ds(pl.multiple_of(j * CHUNK, CHUNK), CHUNK)
        total = out_ref[:, cols].astype(F32)
        for i in range(2):
            k = n_exp + i
            tile = ring[slot, k // 5, 0:ff, (k % 5) * CHUNK:(k % 5 + 1) * CHUNK]
            total = total + jnp.dot(actsh[i], tile, preferred_element_type=F32)
        base[j] = total

        @pl.when(j + 3 < n_chunk)
        def _():
            start(down_copies(slot, j + 3))

        pl.when(j == 0)(lambda: send_sum(0))

        @pl.when(j >= LAG)
        def _():
            pass_on(j - LAG)

    send_sum(n_chunk - 1)

    @pl.loop(n_chunk - LAG, n_chunk)
    def _(j):
        pass_on(j)

    @pl.loop(0, n_chunk)
    def _(j):
        for f, c in enumerate(second_stage(j)):
            c.wait_recv()
            cut = slice(f * side, (f + 1) * side)
            out_ref[:, pl.ds(pl.multiple_of(j * CHUNK + f * side, side), side)] = (base[j, :, cut] + r2[j, f]).astype(BF16)

    for c in rw_copies + [to_mate, x_a, x_b, y_a, y_b, d_a, d_b, m_x, m_y, m_da, m_db]:
        c.wait_send()
    swap(n_chunk - 2).wait_send()
    swap(n_chunk - 1).wait_send()

    @pl.loop(0, n_chunk)
    def _(j):
        for c in first_stage(j) + second_stage(j):
            c.wait_send()


def moe(h, table, resid, eg, eu, ed, sg, su, sd):
    rows, d_model = h.shape
    n_exp, _, ff = eg.shape
    n_chunk = d_model // CHUNK
    slots = 8 * CAP
    vmem = pl.BlockSpec(memory_space=pltpu.VMEM)
    hbm = pl.BlockSpec(memory_space=pl.ANY)
    dma = pltpu.SemaphoreType.DMA
    scratch = [
        pltpu.VMEM((3, 2, d_model, ff), BF16),
        pltpu.VMEM((4, 2 * rows, d_model), BF16),
        pltpu.VMEM((n_exp, slots, d_model), BF16),
        pltpu.VMEM((slots, ff), BF16),
        pltpu.VMEM((2, rows, ff), BF16),
        pltpu.VMEM((n_chunk, 2, 4, rows, CHUNK // 2), F32),
        pltpu.VMEM((n_chunk, 2, 4, rows, CHUNK // 2), F32),
        pltpu.VMEM((n_chunk, 2, 2, rows, CHUNK // 2), F32),
        pltpu.VMEM((n_chunk, 2, rows, CHUNK // 2), F32),
        pltpu.VMEM((2, 2, 4, rows, CHUNK // 2), F32),
        pltpu.VMEM((n_chunk, rows, CHUNK), F32),
        pltpu.VMEM((4, 3, 2 * rows, n_exp * 2 * CAP), BF16),
        pltpu.VMEM((n_exp * 2 * CAP, 2 * rows), F32),
        pltpu.VMEM((4, n_exp * 2 * CAP, 2 * rows), BF16),
        pltpu.VMEM((4, n_exp * 2 * CAP, CHUNK), BF16),
        pltpu.VMEM((4, 2, n_exp, rows), F32),
        dma((3, 10)), dma, dma((11,)), dma((11,)), dma((7,)), dma((7,)), dma((n_chunk,)), dma((n_chunk,)),
        dma((n_chunk, 4)), dma((n_chunk, 4)), dma((n_chunk, 2)), dma((n_chunk, 2)),
    ]
    return pl.pallas_call(
        moe_kernel,
        out_shape=jax.ShapeDtypeStruct((rows, d_model), BF16),
        in_specs=[vmem] * 2 + [hbm] * 7,
        out_specs=vmem,
        scratch_shapes=scratch,
        compiler_params=pltpu.CompilerParams(collective_id=0, has_side_effects=True, vmem_limit_bytes=67043328),
        cost_estimate=pl.CostEstimate(flops=40_000_000_000, bytes_accessed=175_000_000, transcendentals=0),
    )(h, table, resid, eg, eu, ed, sg, su, sd)


def solution(mesh):
    row_one = P(('dp', 'ep'))
    row_two = P(('dp', 'ep'), None)
    row_three = P(('dp', 'ep'), None, None)
    rep_one = P(None)
    rep_two = P(None, None)
    rep_three = P(None, None, None)
    exp_spec = P('ep', None, None)

    def local_step(tok_in, lat_cache, rope_cache, tok_pos, expert_ids, attn_gain, w_query, w_kvdown, w_ukey, w_uval, w_out, ffn_gain, w_router, sh_gate, sh_up, sh_down, ex_gate, ex_up, ex_down):
        resid_bf, h_norm, table, lat_out, rope_out = attention(tok_in, lat_cache, rope_cache, tok_pos, expert_ids, attn_gain, w_query, w_kvdown, w_ukey, w_uval, w_out, ffn_gain, w_router)
        out_hidden = moe(h_norm, table, resid_bf, ex_gate, ex_up, ex_down, sh_gate, sh_up, sh_down)
        return out_hidden, lat_out, rope_out

    in_specs = (row_two, row_three, row_three, row_one, row_two, rep_one, rep_two, rep_two, rep_three, rep_three, rep_two, rep_one, rep_two, rep_two, rep_two, rep_two, exp_spec, exp_spec, exp_spec)
    out_specs = (row_two, row_three, row_three)
    return jax.shard_map(local_step, mesh=mesh, in_specs=in_specs, out_specs=out_specs, check_vma=False)
```

```python
import jax
import jax.numpy as jnp
import numpy as np
from jax import lax
from jax.experimental import pallas as pl
from jax.experimental.pallas import tpu as pltpu
from jax.sharding import PartitionSpec as P

ROUTE_SCALE = 2.827
ROPE_BASE = 10000.0
NORM_EPS = 1e-6
CAP = 24
CHUNK = 256
BLK = 16
LAG = 4
F32 = jnp.float32
BF16 = jnp.bfloat16


def attn_kernel(pos_ref, prow_ref, x_ref, gain_ref, ids_ref, fgain_ref, wkv, wq, wuk, wuv, wo, wr, lat_in, rope_in,
                lat_out, rope_out, res_ref, h_ref, rw_ref,
                vkv, vq, vuk, vuv, vo, vr, lat, rop, xn, qlat, qrope, latn, ropen, olat, ohd, w_sem, lat_sem, rope_sem, lo_sem, ro_sem):
    rows, d_model = x_ref.shape
    n_head, nope, rank = wuk.shape
    rdim = rope_in.shape[1]
    seq = lat_in.shape[1]
    qk = nope + rdim
    n_blk = rows // BLK
    scale = qk ** -0.5
    pair = 2 * qk
    n_pair = n_head // 2
    deep = d_model // 2

    def q_copy(m):
        cols = slice(m * pair, (m + 1) * pair)
        return pltpu.make_async_copy(wq.at[:, cols], vq.at[:, cols], w_sem.at[m])

    kv_copy = pltpu.make_async_copy(wkv, vkv, w_sem.at[n_pair])
    uk_copy = pltpu.make_async_copy(wuk, vuk, w_sem.at[n_pair + 1])
    uv_copy = pltpu.make_async_copy(wuv, vuv, w_sem.at[n_pair + 2])
    o_copy = pltpu.make_async_copy(wo, vo, w_sem.at[n_pair + 3])
    r_copy = pltpu.make_async_copy(wr, vr, w_sem.at[n_pair + 4])

    def lat_load(b):
        return pltpu.make_async_copy(lat_in.at[pl.ds(b * BLK, BLK)], lat.at[pl.ds(b * BLK, BLK)], lat_sem.at[b])

    def rope_load(b):
        return pltpu.make_async_copy(rope_in.at[pl.ds(b * BLK, BLK)], rop.at[pl.ds(b * BLK, BLK)], rope_sem.at[b])

    def lat_save(b):
        return pltpu.make_async_copy(lat.at[pl.ds(b * BLK, BLK)], lat_out.at[pl.ds(b * BLK, BLK)], lo_sem.at[b])

    def rope_save(b):
        return pltpu.make_async_copy(rop.at[pl.ds(b * BLK, BLK)], rope_out.at[pl.ds(b * BLK, BLK)], ro_sem.at[b])

    kv_copy.start()
    for m in range(n_pair):
        q_copy(m).start()
        if m == 0:
            uk_copy.start()

    @pl.loop(0, n_blk)
    def _(b):
        lat_load(b).start()
        rope_load(b).start()

    uv_copy.start()
    o_copy.start()
    r_copy.start()

    xw = x_ref[...].astype(F32)
    xn[...] = (xw * lax.rsqrt(jnp.mean(xw * xw, axis=-1, keepdims=True) + NORM_EPS) * gain_ref[...].reshape(1, d_model).astype(F32)).astype(BF16)
    lane = lax.broadcasted_iota(jnp.int32, (rows, 2 * rdim), 1)
    front = lane % rdim < rdim // 2
    low = lane < rdim
    where_in = lane % (rdim // 2)
    freq = jnp.zeros(lane.shape, F32)
    for i in range(rdim // 2):
        freq = jnp.where(where_in == i, np.float32(ROPE_BASE ** (-2.0 * i / rdim)), freq)
    angle = jnp.transpose(jnp.broadcast_to(prow_ref[...].astype(F32), (rows, rows))) * freq
    cos_t = jnp.cos(angle)
    sin_t = jnp.where(front, -jnp.sin(angle), jnp.sin(angle))

    def rotate(v):
        swapped = jnp.where(front, pltpu.roll(v, 2 * rdim - rdim // 2, 1), pltpu.roll(v, rdim // 2, 1))
        return v * cos_t + swapped * sin_t

    kv_copy.wait()
    kv = lax.dot_general(xn[...], vkv[...], (((1,), (1,)), ((), ())), preferred_element_type=F32)
    lat_raw = kv[:, 0:rank]
    latn[...] = (lat_raw * lax.rsqrt(jnp.mean(lat_raw * lat_raw, axis=-1, keepdims=True) + NORM_EPS)).astype(BF16).astype(F32)
    kr = kv[:, rank:rank + rdim]
    ropen[...] = rotate(jnp.concatenate([kr, kr], axis=1)).astype(BF16).astype(F32)

    for m in range(n_pair):
        q_copy(m).wait()
        if m == 0:
            uk_copy.wait()
        qf = jnp.dot(xn[...], vq[:, m * pair:(m + 1) * pair], preferred_element_type=F32).astype(BF16).astype(F32)
        qa, qb, qc = qf[:, 0:nope], qf[:, nope:2 * nope], qf[:, 2 * nope:3 * nope]
        second = pltpu.roll(jnp.where(low, qc, qb), rdim, 1)
        turned = rotate(jnp.where(low, qb, qc))
        qrope[2 * m] = turned[:, 0:rdim].astype(BF16)
        qrope[2 * m + 1] = pltpu.roll(turned, rdim, 1)[:, 0:rdim].astype(BF16)
        qlat[2 * m] = jnp.dot(qa.astype(BF16), vuk[2 * m], preferred_element_type=F32).astype(BF16)
        qlat[2 * m + 1] = jnp.dot(second.astype(BF16), vuk[2 * m + 1], preferred_element_type=F32).astype(BF16)

    grp = BLK * n_head
    row_i = lax.broadcasted_iota(jnp.int32, (grp, grp), 0)
    col_i = lax.broadcasted_iota(jnp.int32, (grp, grp), 1)
    perm = jnp.where(col_i == (row_i % n_head) * BLK + row_i // n_head, 1.0, 0.0).astype(BF16)

    @pl.loop(0, n_blk)
    def _(b):
        t0 = pl.multiple_of(b * BLK, BLK)
        lat_load(b).wait()
        rope_load(b).wait()
        news = jnp.transpose(ropen[pl.ds(t0, BLK), :])
        slane = lax.broadcasted_iota(jnp.int32, (rdim, seq), 1)
        srow = lax.broadcasted_iota(jnp.int32, (16, rank), 0)
        for t in range(BLK):
            p = pos_ref[t0 + t]
            lo = pl.multiple_of((p // 16) * 16, 16)
            old = lat[t0 + t, pl.ds(lo, 16), :]
            lat[t0 + t, pl.ds(lo, 16), :] = jnp.where(srow == p - lo, latn[pl.ds(t0 + t, 1), :], old.astype(F32)).astype(BF16)
            rop[t0 + t] = jnp.where(slane == p, news[0:rdim, t:t + 1], rop[t0 + t].astype(F32)).astype(BF16)
        q_blk = jnp.dot(perm, qlat[:, pl.ds(t0, BLK), :].reshape(grp, rank), preferred_element_type=F32).astype(BF16)
        r_blk = jnp.dot(perm, qrope[:, pl.ds(t0, BLK), :].reshape(grp, rdim), preferred_element_type=F32).astype(BF16)
        klane = lax.broadcasted_iota(jnp.int32, (n_head, seq), 1)
        scores = []
        for t in range(BLK):
            s = lax.dot_general(q_blk[t * n_head:(t + 1) * n_head], lat[t0 + t], (((1,), (1,)), ((), ())), preferred_element_type=F32)
            s = s + jnp.dot(r_blk[t * n_head:(t + 1) * n_head], rop[t0 + t], preferred_element_type=F32)
            scores.append(jnp.where(klane <= pos_ref[t0 + t], s * scale, -jnp.inf))
        sc = jnp.concatenate(scores, axis=0)
        ex = jnp.exp(sc - jnp.max(sc, axis=-1, keepdims=True))
        prob = (ex / jnp.sum(ex, axis=-1, keepdims=True)).astype(BF16)
        outs = [jnp.dot(prob[t * n_head:(t + 1) * n_head], lat[t0 + t], preferred_element_type=F32).astype(BF16) for t in range(BLK)]
        mixed = jnp.dot(perm, jnp.concatenate(outs, axis=0), preferred_element_type=F32).astype(BF16)
        olat[:, pl.ds(t0, BLK), :] = mixed.reshape(n_head, BLK, rank)
        lat_save(b).start()
        rope_save(b).start()

    uv_copy.wait()
    for h in range(n_head):
        ohd[:, h * nope:(h + 1) * nope] = jnp.dot(olat[h], vuv[h], preferred_element_type=F32).astype(BF16)
    o_copy.wait()
    total = jnp.zeros((rows, 1), F32)
    wide = 512
    for n in range(0, d_model, wide):
        part = jnp.dot(ohd[...], vo[:, n:n + wide], preferred_element_type=F32)
        res = (x_ref[:, n:n + wide].astype(F32) + part).astype(BF16)
        res_ref[:, n:n + wide] = res
        resf = res.astype(F32)
        total = total + jnp.sum(resf * resf, axis=-1, keepdims=True)
    fgain = fgain_ref[...].reshape(1, d_model).astype(F32)
    inv = lax.rsqrt(total * (1.0 / d_model) + NORM_EPS)
    for n in range(0, d_model, wide):
        h_ref[n // deep, :, n % deep:n % deep + wide] = (res_ref[:, n:n + wide].astype(F32) * inv * fgain[:, n:n + wide]).astype(BF16)
    r_copy.wait()
    logits = [lax.dot_general(vr[:, k * deep:(k + 1) * deep], h_ref[k], (((1,), (1,)), ((), ())), preferred_element_type=F32) for k in range(2)]
    gate = jax.nn.sigmoid(logits[0] + logits[1])
    want = lax.broadcasted_iota(jnp.int32, gate.shape, 0)
    picked = want == ids_ref[0:1, :]
    for k in range(1, ids_ref.shape[0]):
        picked = picked | (want == ids_ref[k:k + 1, :])
    chosen = jnp.where(picked, gate, 0.0)
    rw_ref[...] = ROUTE_SCALE * chosen / jnp.sum(chosen, axis=0, keepdims=True)

    @pl.loop(0, n_blk)
    def _(b):
        lat_save(b).wait()
        rope_save(b).wait()


def attention(tok_in, lat_cache, rope_cache, tok_pos, expert_ids, attn_gain, w_query, w_kvdown, w_ukey, w_uval, w_out, ffn_gain, w_router):
    rows, d_model = tok_in.shape
    n_head, nope, rank = w_ukey.shape
    seq, rdim = rope_cache.shape[1], rope_cache.shape[2]
    n_exp = w_router.shape[1]
    vmem = pl.BlockSpec(memory_space=pltpu.VMEM)
    smem = pl.BlockSpec(memory_space=pltpu.SMEM)
    hbm = pl.BlockSpec(memory_space=pl.ANY)
    dma = pltpu.SemaphoreType.DMA
    n_blk = rows // BLK
    scratch = [
        pltpu.VMEM((rank + rdim, d_model), BF16),
        pltpu.VMEM(w_query.shape, BF16),
        pltpu.VMEM(w_ukey.shape, BF16),
        pltpu.VMEM(w_uval.shape, BF16),
        pltpu.VMEM(w_out.shape, BF16),
        pltpu.VMEM((n_exp, d_model), BF16),
        pltpu.VMEM(lat_cache.shape, BF16),
        pltpu.VMEM((rows, rdim, seq), BF16),
        pltpu.VMEM((rows, d_model), BF16),
        pltpu.VMEM((n_head, rows, rank), BF16),
        pltpu.VMEM((n_head, rows, rdim), BF16),
        pltpu.VMEM((rows, rank), F32),
        pltpu.VMEM((rows, 2 * rdim), F32),
        pltpu.VMEM((n_head, rows, rank), BF16),
        pltpu.VMEM((rows, n_head * nope), BF16),
        dma((n_head // 2 + 5,)), dma((n_blk,)), dma((n_blk,)), dma((n_blk,)), dma((n_blk,)),
    ]
    lat_out, rope_out, resid, h, table = pl.pallas_call(
        attn_kernel,
        out_shape=(
            jax.ShapeDtypeStruct(lat_cache.shape, BF16),
            jax.ShapeDtypeStruct((rows, rdim, seq), BF16),
            jax.ShapeDtypeStruct((rows, d_model), BF16),
            jax.ShapeDtypeStruct((2, rows, d_model // 2), BF16),
            jax.ShapeDtypeStruct((n_exp, rows), F32),
        ),
        in_specs=[smem] + [vmem] * 5 + [hbm] * 8,
        out_specs=(hbm, hbm, vmem, vmem, vmem),
        scratch_shapes=scratch,
        compiler_params=pltpu.CompilerParams(vmem_limit_bytes=64000000),
        cost_estimate=pl.CostEstimate(flops=5_000_000_000, bytes_accessed=66_000_000, transcendentals=0),
    )(tok_pos, tok_pos[None, :], tok_in, attn_gain, expert_ids.T, ffn_gain,
      w_kvdown.T, w_query, w_ukey, w_uval, w_out, w_router.T, lat_cache, jnp.swapaxes(rope_cache, 1, 2))
    return resid, h, table, lat_out, jnp.swapaxes(rope_out, 1, 2)


def moe_kernel(h_hbm, rw_hbm, res_hbm, eg, eu, ed, sg, su, sd, out_ref,
               ring, hall, xbuf, part, actsh, drecv, r1, r2, stage, pw, pwf, pbuf, rwin, rw_ref,
               ring_sem, in_sem, ag_s, ag_r, rw_s, rw_r, d_s, d_r, s1_s, s1_r, s2_s, s2_r):
    rows = rw_hbm.shape[1]
    half = rows // 2
    deep = h_hbm.shape[2]
    d_model = 2 * deep
    ff = eg.shape[2]
    n_exp = eg.shape[0]
    n_chunk = d_model // CHUNK
    side = CHUNK // 2
    grp = 2 * CAP
    left = ff - deep
    mids = [(n, min(CHUNK, ff - n)) for n in range(0, ff, CHUNK)]
    me = lax.axis_index('ep')
    core = me % 2
    cx = (me // 2) % 2
    cy = me // 4
    mate = me + 1 - 2 * core
    xn = me + 2 - 4 * cx
    yn = me + 4 - 8 * cy
    dg = yn + 2 - 4 * cx
    others = [(0, 1, mate), (1, 0, xn), (1, 1, xn + 1 - 2 * core), (2, 0, yn), (2, 1, yn + 1 - 2 * core), (3, 0, dg), (3, 1, dg + 1 - 2 * core)]

    def remote(src, dst, ssem, rsem, dev):
        return pltpu.make_async_remote_copy(src_ref=src, dst_ref=dst, send_sem=ssem, recv_sem=rsem, device_id={'ep': dev}, device_id_type=pl.DeviceIdType.MESH)

    def start(copies):
        for c in copies:
            c.start()

    def wait(copies):
        for c in copies:
            c.wait()

    step = deep // 2

    def block_copies(slot, gate, up, k, col):
        out = []
        for b, src in enumerate((gate, up)):
            for q in range(2):
                at = pl.ds(pl.multiple_of(k * deep + q * step, step), step)
                out.append(pltpu.make_async_copy(src.at[at, col], ring.at[slot, b, pl.ds(q * step, step), :], ring_sem.at[slot, 2 * b + q]))
        return out

    def half_copies(i):
        e = i % n_exp
        return block_copies(i % 4, eg.at[e], eu.at[e], i // n_exp, slice(None))

    def shared_copies(q, i):
        col = pl.ds(pl.multiple_of(i * ff, side), ff)
        return block_copies(2 * q, sg, su, 0, col) + block_copies(2 * q + 1, sg, su, 1, col)

    def tile(q, g, lo, size):
        return ring.at[2 * q + g // 10, (g // 5) % 2, pl.ds(lo, size), pl.ds((g % 5) * CHUNK, CHUNK)]

    def pair_sem(q, i):
        return ring_sem.at[2 * q + i // 8, i % 8]

    def down_tiles(q, e):
        return tile(q, e, 0, deep), tile(q, n_exp + e // 2, (e % 2) * left, left)

    def down_copies(j):
        q = j % 2
        cols = pl.ds(pl.multiple_of(j * CHUNK, CHUNK), CHUNK)
        out = []
        for e in range(n_exp):
            head, tail = down_tiles(q, e)
            out.append(pltpu.make_async_copy(ed.at[e, pl.ds(0, deep), cols], head, pair_sem(q, 2 * e)))
            out.append(pltpu.make_async_copy(ed.at[e, pl.ds(deep, left), cols], tail, pair_sem(q, 2 * e + 1)))
        return out

    def shared_tiles(q, c, i):
        return tile(q, 3 * c + i, 0, deep), tile(q, 3 * c + 2, i * left, left)

    def shared_down_copies(t):
        out = []
        for c in range(4):
            cols = pl.ds(pl.multiple_of((4 * t + c) * CHUNK, CHUNK), CHUNK)
            for i in range(2):
                head, tail = shared_tiles(t, c, i)
                out.append(pltpu.make_async_copy(sd.at[pl.ds(i * ff, deep), cols], head, pair_sem(t, 4 * c + 2 * i)))
                out.append(pltpu.make_async_copy(sd.at[pl.ds(i * ff + deep, left), cols], tail, pair_sem(t, 4 * c + 2 * i + 1)))
        return out

    barrier = pltpu.get_barrier_semaphore()
    for _, _, dev in others:
        pl.semaphore_signal(barrier, inc=1, device_id={'ep': dev}, device_id_type=pl.DeviceIdType.MESH)
    in_copies = [pltpu.make_async_copy(h_hbm.at[k], hall.at[0, k, pl.ds(0, rows)], in_sem.at[k]) for k in range(2)]
    in_copies.append(pltpu.make_async_copy(rw_hbm, rw_ref, in_sem.at[2]))
    res_copy = pltpu.make_async_copy(res_hbm, out_ref, in_sem.at[3])
    start(in_copies)
    wait(in_copies)
    start(shared_copies(0, 0))
    start(shared_copies(1, 1))
    res_copy.start()
    pl.semaphore_wait(barrier, len(others))

    part_a, part_b = pl.ds(0, half), pl.ds(half, half)
    own, other = pl.ds(0, rows), pl.ds(rows, rows)
    rw_copies = [remote(rw_ref.at[pl.ds(pl.multiple_of(dev * n_exp, n_exp), n_exp), :], rwin.at[r, p], rw_s.at[i], rw_r.at[i], dev) for i, (r, p, dev) in enumerate(others)]

    class Gather:
        def __init__(self, k):
            def hop(i, src, dst, dev):
                return remote(src, dst, ag_s.at[k, i], ag_r.at[k, i], dev)
            self.mate = hop(0, hall.at[0, k, own], hall.at[0, k, other], mate)
            self.x_a = hop(1, hall.at[0, k, part_a], hall.at[1, k, part_a], xn)
            self.x_b = hop(2, hall.at[0, k, part_b], hall.at[1, k, part_b], xn)
            self.y_b = hop(3, hall.at[0, k, part_b], hall.at[2, k, part_b], yn)
            self.y_a = hop(4, hall.at[0, k, part_a], hall.at[2, k, part_a], yn)
            self.d_a = hop(5, hall.at[1, k, part_a], hall.at[3, k, part_a], yn)
            self.d_b = hop(6, hall.at[2, k, part_b], hall.at[3, k, part_b], xn)
            self.m_x = hop(7, hall.at[1, k, own], hall.at[1, k, other], mate)
            self.m_y = hop(8, hall.at[2, k, own], hall.at[2, k, other], mate)
            self.m_da = hop(9, hall.at[3, k, part_a], hall.at[3, k, pl.ds(rows, half)], mate)
            self.m_db = hop(10, hall.at[3, k, part_b], hall.at[3, k, pl.ds(rows + half, half)], mate)

        def send(self):
            start([self.x_a, self.y_b, self.x_b, self.y_a, self.mate])

        def turn(self):
            self.x_a.wait_recv()
            self.d_a.start()
            self.y_b.wait_recv()
            self.d_b.start()

        def share(self):
            self.x_b.wait_recv()
            self.m_x.start()
            self.y_a.wait_recv()
            self.m_y.start()

        def last(self):
            self.d_a.wait_recv()
            self.m_da.start()
            self.d_b.wait_recv()
            self.m_db.start()

        def sends(self):
            return [self.mate, self.x_a, self.x_b, self.y_b, self.y_a, self.d_a, self.d_b, self.m_x, self.m_y, self.m_da, self.m_db]

    ga, gb = Gather(0), Gather(1)
    ga.send()
    start(rw_copies)

    rwin[0, 0] = rw_ref[pl.ds(pl.multiple_of(me * n_exp, n_exp), n_exp), :]
    for c in rw_copies:
        c.wait_recv()

    def tables(r):
        both = jnp.concatenate([rwin[r, 0], rwin[r, 1]], axis=1)
        two = 2 * rows
        t_in = lax.broadcasted_iota(jnp.int32, (two, two), 0)
        t_out = lax.broadcasted_iota(jnp.int32, (two, two), 1)
        ahead = jnp.where((t_in < t_out) & ((t_in < rows) == (t_out < rows)), 1.0, 0.0).astype(BF16)
        picked = both > 0.0
        before = jnp.dot(jnp.where(picked, 1.0, 0.0).astype(BF16), ahead, preferred_element_type=F32)
        lane = lax.broadcasted_iota(jnp.int32, (n_exp, two), 1)
        slot = jnp.where(picked, before + jnp.where(lane < rows, 0.0, float(CAP)), -1.0).astype(jnp.int32)
        want = lax.broadcasted_iota(jnp.int32, (grp, two), 0)
        for e in range(n_exp):
            hit = want == slot[e:e + 1, :]
            pbuf[r, e * grp:(e + 1) * grp, :] = jnp.where(hit, 1.0, 0.0).astype(BF16)
            pwf[e * grp:(e + 1) * grp, :] = jnp.where(hit, both[e:e + 1, :], 0.0)
        turned = pwf[...].T
        hi = turned.astype(BF16)
        rest = turned - hi.astype(F32)
        mid = rest.astype(BF16)
        pw[r, 0] = hi
        pw[r, 1] = mid
        pw[r, 2] = (rest - mid.astype(F32)).astype(BF16)

    def gather_rows(r, k):
        wide = 512
        for n in range(0, deep, wide):
            got = jnp.dot(pbuf[r], hall[r, k, :, n:n + wide], preferred_element_type=F32).astype(BF16)
            for e in range(n_exp):
                xbuf[k, e, r * grp:(r + 1) * grp, n:n + wide] = got[e * grp:(e + 1) * grp, :]

    def shared_hidden(i):
        wait(shared_copies(i, i))
        for n, w in mids:
            vals = []
            for b in range(2):
                v = jnp.dot(hall[0, 0, 0:rows, :], ring[2 * i, b, :, n:n + w], preferred_element_type=F32)
                vals.append(v + jnp.dot(hall[0, 1, 0:rows, :], ring[2 * i + 1, b, :, n:n + w], preferred_element_type=F32))
            actsh[i, :, n:n + w] = (jax.nn.silu(vals[0]) * vals[1]).astype(BF16)
        for k in range(2):
            start(half_copies(2 * i + k))

    for r in range(4):
        tables(r)
    ga.turn()
    gb.send()
    shared_hidden(0)
    ga.share()
    ga.mate.wait_recv()
    gather_rows(0, 0)
    shared_hidden(1)
    ga.last()
    ga.m_x.wait_recv()
    gather_rows(1, 0)
    ga.m_y.wait_recv()
    gather_rows(2, 0)
    ga.m_da.wait_recv()
    ga.m_db.wait_recv()
    gather_rows(3, 0)

    @pl.loop(0, n_exp)
    def _(e):
        slot = e % 4
        wait(half_copies(e))
        for n, w in mids:
            part[e, :, n:n + w] = jnp.dot(xbuf[0, e], ring[slot, 0, :, n:n + w], preferred_element_type=F32)
            part[e, :, ff + n:ff + n + w] = jnp.dot(xbuf[0, e], ring[slot, 1, :, n:n + w], preferred_element_type=F32)
        start(half_copies(e + 4))

        @pl.when(e == 0)
        def _():
            gb.turn()
            gb.mate.wait_recv()
            gather_rows(0, 1)

        @pl.when(e == 2)
        def _():
            gb.share()

        @pl.when(e == 3)
        def _():
            gb.m_x.wait_recv()
            gather_rows(1, 1)
            gb.m_y.wait_recv()
            gather_rows(2, 1)

        pl.when(e == 4)(gb.last)

        @pl.when(e == 5)
        def _():
            gb.m_da.wait_recv()
            gb.m_db.wait_recv()
            gather_rows(3, 1)

    @pl.loop(0, n_exp)
    def _(e):
        slot = e % 4
        wait(half_copies(n_exp + e))
        late = []
        for n, w in mids:
            g = part[e, :, n:n + w] + jnp.dot(xbuf[1, e], ring[slot, 0, :, n:n + w], preferred_element_type=F32)
            u = part[e, :, ff + n:ff + n + w] + jnp.dot(xbuf[1, e], ring[slot, 1, :, n:n + w], preferred_element_type=F32)
            act = (jax.nn.silu(g) * u).astype(BF16)
            if n < deep:
                xbuf[0, e, :, n:n + w] = act
            else:
                late.append((n - deep, w, act))
        for n, w, act in late:
            xbuf[1, e, :, n:n + w] = act
        pl.when(e < 4)(lambda: start(half_copies(n_exp + e + 4)))
        pl.when(e == 5)(lambda: start(down_copies(0)))
        pl.when(e == 7)(lambda: start(down_copies(1)))

    def acc(j, f, r):
        return part.at[j, pl.ds(0, rows), pl.ds((4 * f + r) * side, side)]

    def base(j, f):
        return part.at[j, pl.ds(0, rows), pl.ds((8 + f) * side, side)]

    def first_stage(j):
        out = []
        for f, dev in enumerate((xn, yn)):
            for q, r in enumerate((1 + f, 3)):
                out.append(remote(acc(j, f, r), r1.at[j, f, q], s1_s.at[j, 2 * f + q], s1_r.at[j, 2 * f + q], dev))
        return out

    def second_stage(j):
        return [remote(acc(j, f, 2 - f), r2.at[j, f], s2_s.at[j, f], s2_r.at[j, f], dev) for f, dev in enumerate((yn, xn))]

    def swap(j):
        return remote(stage.at[j % 2], drecv.at[j], d_s.at[j], d_r.at[j], mate)

    def send_sum(j):
        swap(j).wait_recv()
        for f in range(2):
            for r in range(4):
                acc(j, f, r)[...] = acc(j, f, r)[...] + drecv[j, f, r]
        start(first_stage(j))

    def pass_on(j):
        for c in first_stage(j):
            c.wait_recv()
        for f, c in enumerate(second_stage(j)):
            acc(j, f, 2 - f)[...] = acc(j, f, 2 - f)[...] + r1[j, f, 1]
            c.start()
        for f in range(2):
            acc(j, f, 0)[...] = acc(j, f, 0)[...] + r1[j, f, 0]

    @pl.loop(0, n_chunk)
    def _(j):
        q = j % 2
        wait(down_copies(j))
        for e in range(n_exp):
            if e == 3:
                pl.when(j >= 1)(lambda: send_sum(j - 1))
            head, tail = down_tiles(q, e)
            got = jnp.dot(xbuf[0, e], head[...], preferred_element_type=F32)
            got = (got + jnp.dot(xbuf[1, e, :, 0:left], tail[...], preferred_element_type=F32)).astype(BF16)
            for r in range(4):
                pbuf[r, e * grp:(e + 1) * grp, :] = got[r * grp:(r + 1) * grp, :]
        pl.when(j >= 2)(lambda: swap(j - 2).wait_send())
        for r in range(4):
            out = jnp.dot(pw[r, 0], pbuf[r], preferred_element_type=F32)
            out = out + jnp.dot(pw[r, 1], pbuf[r], preferred_element_type=F32)
            out = out + jnp.dot(pw[r, 2], pbuf[r], preferred_element_type=F32)
            for f in range(2):
                cut = slice(f * side, (f + 1) * side)
                acc(j, f, r)[...] = out[0:rows, cut]
                stage[q, f, r] = out[rows:, cut]
        swap(j).start()
        pl.when(j + 2 < n_chunk)(lambda: start(down_copies(j + 2)))
        pl.when(j == n_chunk - 2)(lambda: start(shared_down_copies(0)))
        pl.when(j == n_chunk - 1)(lambda: start(shared_down_copies(1)))
        pl.when(j >= LAG)(lambda: pass_on(j - LAG))

    send_sum(n_chunk - 1)
    pass_on(n_chunk - 4)
    pass_on(n_chunk - 3)


    res_copy.wait()

    @pl.loop(0, 2)
    def _(t):
        wait(shared_down_copies(t))
        for c in range(4):
            j = 4 * t + c
            cols = pl.ds(pl.multiple_of(j * CHUNK, CHUNK), CHUNK)
            total = out_ref[:, cols].astype(F32)
            for i in range(2):
                head, tail = shared_tiles(t, c, i)
                total = total + jnp.dot(actsh[i, :, 0:deep], head[...], preferred_element_type=F32)
                total = total + jnp.dot(actsh[i, :, deep:ff], tail[...], preferred_element_type=F32)
            for f in range(2):
                base(j, f)[...] = total[:, f * side:(f + 1) * side]
        pass_on(n_chunk - 2 + t)

    @pl.loop(0, n_chunk)
    def _(j):
        for f, c in enumerate(second_stage(j)):
            c.wait_recv()
            cols = pl.ds(pl.multiple_of(j * CHUNK + f * side, side), side)
            out_ref[:, cols] = (base(j, f)[...] + (acc(j, f, 0)[...] + r2[j, f])).astype(BF16)

    for c in rw_copies + ga.sends() + gb.sends():
        c.wait_send()
    swap(n_chunk - 2).wait_send()
    swap(n_chunk - 1).wait_send()

    @pl.loop(0, n_chunk)
    def _(j):
        for c in first_stage(j) + second_stage(j):
            c.wait_send()


def moe(h, table, resid, eg, eu, ed, sg, su, sd):
    _, rows, deep = h.shape
    d_model = 2 * deep
    n_exp, _, ff = eg.shape
    n_chunk = d_model // CHUNK
    side = CHUNK // 2
    slots = 8 * CAP
    pairs = 2 * CAP * n_exp
    vmem = pl.BlockSpec(memory_space=pltpu.VMEM)
    hbm = pl.BlockSpec(memory_space=pl.ANY)
    dma = pltpu.SemaphoreType.DMA
    scratch = [
        pltpu.VMEM((4, 2, deep, ff), BF16),
        pltpu.VMEM((4, 2, 2 * rows, deep), BF16),
        pltpu.VMEM((2, n_exp, slots, deep), BF16),
        pltpu.VMEM((n_exp, slots, 2 * ff), F32),
        pltpu.VMEM((2, rows, ff), BF16),
        pltpu.VMEM((n_chunk, 2, 4, rows, side), F32),
        pltpu.VMEM((n_chunk, 2, 2, rows, side), F32),
        pltpu.VMEM((n_chunk, 2, rows, side), F32),
        pltpu.VMEM((2, 2, 4, rows, side), F32),
        pltpu.VMEM((4, 3, 2 * rows, pairs), BF16),
        pltpu.VMEM((pairs, 2 * rows), F32),
        pltpu.VMEM((4, pairs, 2 * rows), BF16),
        pltpu.VMEM((4, 2, n_exp, rows), F32),
        pltpu.VMEM(table.shape, F32),
        dma((4, 8)), dma((4,)), dma((2, 11)), dma((2, 11)), dma((7,)), dma((7,)), dma((n_chunk,)), dma((n_chunk,)),
        dma((n_chunk, 4)), dma((n_chunk, 4)), dma((n_chunk, 2)), dma((n_chunk, 2)),
    ]
    return pl.pallas_call(
        moe_kernel,
        out_shape=jax.ShapeDtypeStruct((rows, d_model), BF16),
        in_specs=[hbm] * 9,
        out_specs=vmem,
        scratch_shapes=scratch,
        compiler_params=pltpu.CompilerParams(collective_id=0, has_side_effects=True, vmem_limit_bytes=67043328),
        cost_estimate=pl.CostEstimate(flops=40_000_000_000, bytes_accessed=175_000_000, transcendentals=0),
    )(h, table, resid, eg, eu, ed, sg, su, sd)


def solution(mesh):
    row_one = P(('dp', 'ep'))
    row_two = P(('dp', 'ep'), None)
    row_three = P(('dp', 'ep'), None, None)
    rep_one = P(None)
    rep_two = P(None, None)
    rep_three = P(None, None, None)
    exp_spec = P('ep', None, None)

    def local_step(tok_in, lat_cache, rope_cache, tok_pos, expert_ids, attn_gain, w_query, w_kvdown, w_ukey, w_uval, w_out, ffn_gain, w_router, sh_gate, sh_up, sh_down, ex_gate, ex_up, ex_down):
        resid_bf, h_norm, table, lat_out, rope_out = attention(tok_in, lat_cache, rope_cache, tok_pos, expert_ids, attn_gain, w_query, w_kvdown, w_ukey, w_uval, w_out, ffn_gain, w_router)
        out_hidden = moe(h_norm, table, resid_bf, ex_gate, ex_up, ex_down, sh_gate, sh_up, sh_down)
        return out_hidden, lat_out, rope_out

    in_specs = (row_two, row_three, row_three, row_one, row_two, rep_one, rep_two, rep_two, rep_three, rep_three, rep_two, rep_one, rep_two, rep_two, rep_two, rep_two, exp_spec, exp_spec, exp_spec)
    out_specs = (row_two, row_three, row_three)
    return jax.shard_map(local_step, mesh=mesh, in_specs=in_specs, out_specs=out_specs, check_vma=False)
```

```python
import jax
import jax.numpy as jnp
import numpy as np
from jax import lax
from jax.experimental import pallas as pl
from jax.experimental.pallas import tpu as pltpu
from jax.sharding import PartitionSpec as P

ROUTE_SCALE = 2.827
ROPE_BASE = 10000.0
NORM_EPS = 1e-6
CAP = 24
CHUNK = 256
BLK = 16
LAG = 2
F32 = jnp.float32
BF16 = jnp.bfloat16


def attn_kernel(pos_ref, prow_ref, x_ref, gain_ref, ids_ref, fgain_ref, wkv, wq, wuk, wuv, wo, wr, lat_in, rope_in,
                lat_out, rope_out, res_ref, h_ref, rw_ref,
                vkv, vq, vuk, vuv, vo, vr, lat, rop, xn, qlat, qrope, latn, ropen, olat, ohd, w_sem, lat_sem, rope_sem, lo_sem, ro_sem):
    rows, d_model = x_ref.shape
    n_head, nope, rank = wuk.shape
    rdim = rope_in.shape[1]
    seq = lat_in.shape[1]
    qk = nope + rdim
    n_blk = rows // BLK
    scale = qk ** -0.5
    pair = 2 * qk
    n_pair = n_head // 2
    deep = d_model // 2

    def q_copy(m):
        cols = slice(m * pair, (m + 1) * pair)
        return pltpu.make_async_copy(wq.at[:, cols], vq.at[:, cols], w_sem.at[m])

    kv_copy = pltpu.make_async_copy(wkv, vkv, w_sem.at[n_pair])
    uk_copy = pltpu.make_async_copy(wuk, vuk, w_sem.at[n_pair + 1])
    uv_copy = pltpu.make_async_copy(wuv, vuv, w_sem.at[n_pair + 2])
    o_copy = pltpu.make_async_copy(wo, vo, w_sem.at[n_pair + 3])
    r_copy = pltpu.make_async_copy(wr, vr, w_sem.at[n_pair + 4])

    def lat_load(b):
        return pltpu.make_async_copy(lat_in.at[pl.ds(b * BLK, BLK)], lat.at[pl.ds(b * BLK, BLK)], lat_sem.at[b])

    def rope_load(b):
        return pltpu.make_async_copy(rope_in.at[pl.ds(b * BLK, BLK)], rop.at[pl.ds(b * BLK, BLK)], rope_sem.at[b])

    def lat_save(b):
        return pltpu.make_async_copy(lat.at[pl.ds(b * BLK, BLK)], lat_out.at[pl.ds(b * BLK, BLK)], lo_sem.at[b])

    def rope_save(b):
        return pltpu.make_async_copy(rop.at[pl.ds(b * BLK, BLK)], rope_out.at[pl.ds(b * BLK, BLK)], ro_sem.at[b])

    kv_copy.start()
    for m in range(n_pair):
        q_copy(m).start()
        if m == 0:
            uk_copy.start()

    @pl.loop(0, n_blk)
    def _(b):
        lat_load(b).start()
        rope_load(b).start()

    uv_copy.start()
    o_copy.start()
    r_copy.start()

    xw = x_ref[...].astype(F32)
    xn[...] = (xw * lax.rsqrt(jnp.mean(xw * xw, axis=-1, keepdims=True) + NORM_EPS) * gain_ref[...].reshape(1, d_model).astype(F32)).astype(BF16)
    lane = lax.broadcasted_iota(jnp.int32, (rows, 2 * rdim), 1)
    front = lane % rdim < rdim // 2
    low = lane < rdim
    where_in = lane % (rdim // 2)
    freq = jnp.zeros(lane.shape, F32)
    for i in range(rdim // 2):
        freq = jnp.where(where_in == i, np.float32(ROPE_BASE ** (-2.0 * i / rdim)), freq)
    angle = jnp.transpose(jnp.broadcast_to(prow_ref[...].astype(F32), (rows, rows))) * freq
    cos_t = jnp.cos(angle)
    sin_t = jnp.where(front, -jnp.sin(angle), jnp.sin(angle))

    def rotate(v):
        swapped = jnp.where(front, pltpu.roll(v, 2 * rdim - rdim // 2, 1), pltpu.roll(v, rdim // 2, 1))
        return v * cos_t + swapped * sin_t

    kv_copy.wait()
    kv = lax.dot_general(xn[...], vkv[...], (((1,), (1,)), ((), ())), preferred_element_type=F32)
    lat_raw = kv[:, 0:rank]
    latn[...] = (lat_raw * lax.rsqrt(jnp.mean(lat_raw * lat_raw, axis=-1, keepdims=True) + NORM_EPS)).astype(BF16).astype(F32)
    kr = kv[:, rank:rank + rdim]
    ropen[...] = rotate(jnp.concatenate([kr, kr], axis=1)).astype(BF16).astype(F32)

    for m in range(n_pair):
        q_copy(m).wait()
        if m == 0:
            uk_copy.wait()
        qf = jnp.dot(xn[...], vq[:, m * pair:(m + 1) * pair], preferred_element_type=F32).astype(BF16).astype(F32)
        qa, qb, qc = qf[:, 0:nope], qf[:, nope:2 * nope], qf[:, 2 * nope:3 * nope]
        second = pltpu.roll(jnp.where(low, qc, qb), rdim, 1)
        turned = rotate(jnp.where(low, qb, qc))
        qrope[2 * m] = turned[:, 0:rdim].astype(BF16)
        qrope[2 * m + 1] = pltpu.roll(turned, rdim, 1)[:, 0:rdim].astype(BF16)
        qlat[2 * m] = jnp.dot(qa.astype(BF16), vuk[2 * m], preferred_element_type=F32).astype(BF16)
        qlat[2 * m + 1] = jnp.dot(second.astype(BF16), vuk[2 * m + 1], preferred_element_type=F32).astype(BF16)

    grp = BLK * n_head
    row_i = lax.broadcasted_iota(jnp.int32, (grp, grp), 0)
    col_i = lax.broadcasted_iota(jnp.int32, (grp, grp), 1)
    perm = jnp.where(col_i == (row_i % n_head) * BLK + row_i // n_head, 1.0, 0.0).astype(BF16)

    @pl.loop(0, n_blk)
    def _(b):
        t0 = pl.multiple_of(b * BLK, BLK)
        lat_load(b).wait()
        rope_load(b).wait()
        news = jnp.transpose(ropen[pl.ds(t0, BLK), :])
        slane = lax.broadcasted_iota(jnp.int32, (rdim, seq), 1)
        srow = lax.broadcasted_iota(jnp.int32, (16, rank), 0)
        for t in range(BLK):
            p = pos_ref[t0 + t]
            lo = pl.multiple_of((p // 16) * 16, 16)
            old = lat[t0 + t, pl.ds(lo, 16), :]
            lat[t0 + t, pl.ds(lo, 16), :] = jnp.where(srow == p - lo, latn[pl.ds(t0 + t, 1), :], old.astype(F32)).astype(BF16)
            rop[t0 + t] = jnp.where(slane == p, news[0:rdim, t:t + 1], rop[t0 + t].astype(F32)).astype(BF16)
        q_blk = jnp.dot(perm, qlat[:, pl.ds(t0, BLK), :].reshape(grp, rank), preferred_element_type=F32).astype(BF16)
        r_blk = jnp.dot(perm, qrope[:, pl.ds(t0, BLK), :].reshape(grp, rdim), preferred_element_type=F32).astype(BF16)
        klane = lax.broadcasted_iota(jnp.int32, (n_head, seq), 1)
        scores = []
        for t in range(BLK):
            s = lax.dot_general(q_blk[t * n_head:(t + 1) * n_head], lat[t0 + t], (((1,), (1,)), ((), ())), preferred_element_type=F32)
            s = s + jnp.dot(r_blk[t * n_head:(t + 1) * n_head], rop[t0 + t], preferred_element_type=F32)
            scores.append(jnp.where(klane <= pos_ref[t0 + t], s * scale, -jnp.inf))
        sc = jnp.concatenate(scores, axis=0)
        ex = jnp.exp(sc - jnp.max(sc, axis=-1, keepdims=True))
        prob = (ex / jnp.sum(ex, axis=-1, keepdims=True)).astype(BF16)
        outs = [jnp.dot(prob[t * n_head:(t + 1) * n_head], lat[t0 + t], preferred_element_type=F32).astype(BF16) for t in range(BLK)]
        mixed = jnp.dot(perm, jnp.concatenate(outs, axis=0), preferred_element_type=F32).astype(BF16)
        olat[:, pl.ds(t0, BLK), :] = mixed.reshape(n_head, BLK, rank)
        lat_save(b).start()
        rope_save(b).start()

    uv_copy.wait()
    for h in range(n_head):
        ohd[:, h * nope:(h + 1) * nope] = jnp.dot(olat[h], vuv[h], preferred_element_type=F32).astype(BF16)
    o_copy.wait()
    total = jnp.zeros((rows, 1), F32)
    wide = 512
    for n in range(0, d_model, wide):
        part = jnp.dot(ohd[...], vo[:, n:n + wide], preferred_element_type=F32)
        res = (x_ref[:, n:n + wide].astype(F32) + part).astype(BF16)
        res_ref[:, n:n + wide] = res
        resf = res.astype(F32)
        total = total + jnp.sum(resf * resf, axis=-1, keepdims=True)
    fgain = fgain_ref[...].reshape(1, d_model).astype(F32)
    inv = lax.rsqrt(total * (1.0 / d_model) + NORM_EPS)
    for n in range(0, d_model, wide):
        h_ref[n // deep, :, n % deep:n % deep + wide] = (res_ref[:, n:n + wide].astype(F32) * inv * fgain[:, n:n + wide]).astype(BF16)
    r_copy.wait()
    logits = [lax.dot_general(vr[:, k * deep:(k + 1) * deep], h_ref[k], (((1,), (1,)), ((), ())), preferred_element_type=F32) for k in range(2)]
    gate = jax.nn.sigmoid(logits[0] + logits[1])
    want = lax.broadcasted_iota(jnp.int32, gate.shape, 0)
    picked = want == ids_ref[0:1, :]
    for k in range(1, ids_ref.shape[0]):
        picked = picked | (want == ids_ref[k:k + 1, :])
    chosen = jnp.where(picked, gate, 0.0)
    rw_ref[...] = ROUTE_SCALE * chosen / jnp.sum(chosen, axis=0, keepdims=True)

    @pl.loop(0, n_blk)
    def _(b):
        lat_save(b).wait()
        rope_save(b).wait()


def attention(tok_in, lat_cache, rope_cache, tok_pos, expert_ids, attn_gain, w_query, w_kvdown, w_ukey, w_uval, w_out, ffn_gain, w_router):
    rows, d_model = tok_in.shape
    n_head, nope, rank = w_ukey.shape
    seq, rdim = rope_cache.shape[1], rope_cache.shape[2]
    n_exp = w_router.shape[1]
    vmem = pl.BlockSpec(memory_space=pltpu.VMEM)
    smem = pl.BlockSpec(memory_space=pltpu.SMEM)
    hbm = pl.BlockSpec(memory_space=pl.ANY)
    dma = pltpu.SemaphoreType.DMA
    n_blk = rows // BLK
    scratch = [
        pltpu.VMEM((rank + rdim, d_model), BF16),
        pltpu.VMEM(w_query.shape, BF16),
        pltpu.VMEM(w_ukey.shape, BF16),
        pltpu.VMEM(w_uval.shape, BF16),
        pltpu.VMEM(w_out.shape, BF16),
        pltpu.VMEM((n_exp, d_model), BF16),
        pltpu.VMEM(lat_cache.shape, BF16),
        pltpu.VMEM((rows, rdim, seq), BF16),
        pltpu.VMEM((rows, d_model), BF16),
        pltpu.VMEM((n_head, rows, rank), BF16),
        pltpu.VMEM((n_head, rows, rdim), BF16),
        pltpu.VMEM((rows, rank), F32),
        pltpu.VMEM((rows, 2 * rdim), F32),
        pltpu.VMEM((n_head, rows, rank), BF16),
        pltpu.VMEM((rows, n_head * nope), BF16),
        dma((n_head // 2 + 5,)), dma((n_blk,)), dma((n_blk,)), dma((n_blk,)), dma((n_blk,)),
    ]
    lat_out, rope_out, resid, h, table = pl.pallas_call(
        attn_kernel,
        out_shape=(
            jax.ShapeDtypeStruct(lat_cache.shape, BF16),
            jax.ShapeDtypeStruct((rows, rdim, seq), BF16),
            jax.ShapeDtypeStruct((rows, d_model), BF16),
            jax.ShapeDtypeStruct((2, rows, d_model // 2), BF16),
            jax.ShapeDtypeStruct((n_exp, rows), F32),
        ),
        in_specs=[smem] + [vmem] * 5 + [hbm] * 8,
        out_specs=(hbm, hbm, vmem, vmem, vmem),
        scratch_shapes=scratch,
        compiler_params=pltpu.CompilerParams(vmem_limit_bytes=64000000),
        cost_estimate=pl.CostEstimate(flops=5_000_000_000, bytes_accessed=66_000_000, transcendentals=0),
    )(tok_pos, tok_pos[None, :], tok_in, attn_gain, expert_ids.T, ffn_gain,
      w_kvdown.T, w_query, w_ukey, w_uval, w_out, w_router.T, lat_cache, jnp.swapaxes(rope_cache, 1, 2))
    return resid, h, table, lat_out, jnp.swapaxes(rope_out, 1, 2)


def moe_kernel(h_hbm, rw_hbm, res_hbm, eg, eu, ed, sg, su, sd, out_ref,
               ring, hall, xbuf, part, actsh, drecv, r1, r2, stage, pw, pwf, pbuf, rwin, rw_ref,
               ring_sem, in_sem, ag_s, ag_r, rw_s, rw_r, d_s, d_r, s1_s, s1_r, s2_s, s2_r):
    rows = rw_hbm.shape[1]
    half = rows // 2
    deep = h_hbm.shape[2]
    d_model = 2 * deep
    ff = eg.shape[2]
    n_exp = eg.shape[0]
    n_chunk = d_model // CHUNK
    side = CHUNK // 2
    grp = 2 * CAP
    left = ff - deep
    mids = [(n, min(CHUNK, ff - n)) for n in range(0, ff, CHUNK)]
    me = lax.axis_index('ep')
    core = me % 2
    cx = (me // 2) % 2
    cy = me // 4
    mate = me + 1 - 2 * core
    xn = me + 2 - 4 * cx
    yn = me + 4 - 8 * cy
    dg = yn + 2 - 4 * cx
    others = [(0, 1, mate), (1, 0, xn), (1, 1, xn + 1 - 2 * core), (2, 0, yn), (2, 1, yn + 1 - 2 * core), (3, 0, dg), (3, 1, dg + 1 - 2 * core)]

    def remote(src, dst, ssem, rsem, dev):
        return pltpu.make_async_remote_copy(src_ref=src, dst_ref=dst, send_sem=ssem, recv_sem=rsem, device_id={'ep': dev}, device_id_type=pl.DeviceIdType.MESH)

    def start(copies):
        for c in copies:
            c.start()

    def wait(copies):
        for c in copies:
            c.wait()

    step = deep // 2

    def block_copies(slot, gate, up, k, col):
        out = []
        for b, src in enumerate((gate, up)):
            for q in range(2):
                at = pl.ds(pl.multiple_of(k * deep + q * step, step), step)
                out.append(pltpu.make_async_copy(src.at[at, col], ring.at[slot, b, pl.ds(q * step, step), :], ring_sem.at[slot, 2 * b + q]))
        return out

    def half_copies(i):
        e = i % n_exp
        return block_copies(i % 4, eg.at[e], eu.at[e], i // n_exp, slice(None))

    def shared_copies(q, i):
        col = pl.ds(pl.multiple_of(i * ff, side), ff)
        return block_copies(2 * q, sg, su, 0, col) + block_copies(2 * q + 1, sg, su, 1, col)

    def tile(q, g, lo, size):
        return ring.at[2 * q + g // 10, (g // 5) % 2, pl.ds(lo, size), pl.ds((g % 5) * CHUNK, CHUNK)]

    def pair_sem(q, i):
        return ring_sem.at[2 * q + i // 8, i % 8]

    def down_tiles(q, e):
        return tile(q, e, 0, deep), tile(q, n_exp + e // 2, (e % 2) * left, left)

    def down_copies(j):
        q = j % 2
        cols = pl.ds(pl.multiple_of(j * CHUNK, CHUNK), CHUNK)
        out = []
        for e in range(n_exp):
            head, tail = down_tiles(q, e)
            out.append(pltpu.make_async_copy(ed.at[e, pl.ds(0, deep), cols], head, pair_sem(q, 2 * e)))
            out.append(pltpu.make_async_copy(ed.at[e, pl.ds(deep, left), cols], tail, pair_sem(q, 2 * e + 1)))
        return out

    def shared_tiles(q, c, i):
        return tile(q, 3 * c + i, 0, deep), tile(q, 3 * c + 2, i * left, left)

    def shared_down_copies(t):
        out = []
        for c in range(4):
            cols = pl.ds(pl.multiple_of((4 * t + c) * CHUNK, CHUNK), CHUNK)
            for i in range(2):
                head, tail = shared_tiles(t, c, i)
                out.append(pltpu.make_async_copy(sd.at[pl.ds(i * ff, deep), cols], head, pair_sem(t, 4 * c + 2 * i)))
                out.append(pltpu.make_async_copy(sd.at[pl.ds(i * ff + deep, left), cols], tail, pair_sem(t, 4 * c + 2 * i + 1)))
        return out

    barrier = pltpu.get_barrier_semaphore()
    for _, _, dev in others:
        pl.semaphore_signal(barrier, inc=1, device_id={'ep': dev}, device_id_type=pl.DeviceIdType.MESH)
    in_copies = [pltpu.make_async_copy(h_hbm.at[k], hall.at[0, k, pl.ds(0, rows)], in_sem.at[k]) for k in range(2)]
    in_copies.append(pltpu.make_async_copy(rw_hbm, rw_ref, in_sem.at[2]))
    res_copy = pltpu.make_async_copy(res_hbm, out_ref, in_sem.at[3])
    start(in_copies)
    wait(in_copies)
    start(shared_copies(0, 0))
    start(shared_copies(1, 1))
    res_copy.start()
    pl.semaphore_wait(barrier, len(others))

    part_a, part_b = pl.ds(0, half), pl.ds(half, half)
    own, other = pl.ds(0, rows), pl.ds(rows, rows)
    rw_copies = [remote(rw_ref.at[pl.ds(pl.multiple_of(dev * n_exp, n_exp), n_exp), :], rwin.at[r, p], rw_s.at[i], rw_r.at[i], dev) for i, (r, p, dev) in enumerate(others)]

    class Gather:
        def __init__(self, k):
            def hop(i, src, dst, dev):
                return remote(src, dst, ag_s.at[k, i], ag_r.at[k, i], dev)
            self.mate = hop(0, hall.at[0, k, own], hall.at[0, k, other], mate)
            self.x_a = hop(1, hall.at[0, k, part_a], hall.at[1, k, part_a], xn)
            self.x_b = hop(2, hall.at[0, k, part_b], hall.at[1, k, part_b], xn)
            self.y_b = hop(3, hall.at[0, k, part_b], hall.at[2, k, part_b], yn)
            self.y_a = hop(4, hall.at[0, k, part_a], hall.at[2, k, part_a], yn)
            self.d_a = hop(5, hall.at[1, k, part_a], hall.at[3, k, part_a], yn)
            self.d_b = hop(6, hall.at[2, k, part_b], hall.at[3, k, part_b], xn)
            self.m_x = hop(7, hall.at[1, k, own], hall.at[1, k, other], mate)
            self.m_y = hop(8, hall.at[2, k, own], hall.at[2, k, other], mate)
            self.m_da = hop(9, hall.at[3, k, part_a], hall.at[3, k, pl.ds(rows, half)], mate)
            self.m_db = hop(10, hall.at[3, k, part_b], hall.at[3, k, pl.ds(rows + half, half)], mate)

        def send(self):
            start([self.x_a, self.y_b, self.x_b, self.y_a, self.mate])

        def turn(self):
            self.x_a.wait_recv()
            self.d_a.start()
            self.y_b.wait_recv()
            self.d_b.start()

        def share(self):
            self.x_b.wait_recv()
            self.m_x.start()
            self.y_a.wait_recv()
            self.m_y.start()

        def last(self):
            self.d_a.wait_recv()
            self.m_da.start()
            self.d_b.wait_recv()
            self.m_db.start()

        def sends(self):
            return [self.mate, self.x_a, self.x_b, self.y_b, self.y_a, self.d_a, self.d_b, self.m_x, self.m_y, self.m_da, self.m_db]

    ga, gb = Gather(0), Gather(1)
    ga.send()
    start(rw_copies)

    rwin[0, 0] = rw_ref[pl.ds(pl.multiple_of(me * n_exp, n_exp), n_exp), :]
    for c in rw_copies:
        c.wait_recv()

    def tables(r):
        both = jnp.concatenate([rwin[r, 0], rwin[r, 1]], axis=1)
        two = 2 * rows
        t_in = lax.broadcasted_iota(jnp.int32, (two, two), 0)
        t_out = lax.broadcasted_iota(jnp.int32, (two, two), 1)
        ahead = jnp.where((t_in < t_out) & ((t_in < rows) == (t_out < rows)), 1.0, 0.0).astype(BF16)
        picked = both > 0.0
        before = jnp.dot(jnp.where(picked, 1.0, 0.0).astype(BF16), ahead, preferred_element_type=F32)
        lane = lax.broadcasted_iota(jnp.int32, (n_exp, two), 1)
        slot = jnp.where(picked, before + jnp.where(lane < rows, 0.0, float(CAP)), -1.0).astype(jnp.int32)
        want = lax.broadcasted_iota(jnp.int32, (grp, two), 0)
        for e in range(n_exp):
            hit = want == slot[e:e + 1, :]
            pbuf[r, e * grp:(e + 1) * grp, :] = jnp.where(hit, 1.0, 0.0).astype(BF16)
            pwf[e * grp:(e + 1) * grp, :] = jnp.where(hit, both[e:e + 1, :], 0.0)
        turned = pwf[...].T
        hi = turned.astype(BF16)
        rest = turned - hi.astype(F32)
        mid = rest.astype(BF16)
        pw[r, 0] = hi
        pw[r, 1] = mid
        pw[r, 2] = (rest - mid.astype(F32)).astype(BF16)

    def gather_rows(r, k):
        wide = 512
        for n in range(0, deep, wide):
            got = jnp.dot(pbuf[r], hall[r, k, :, n:n + wide], preferred_element_type=F32).astype(BF16)
            for e in range(n_exp):
                xbuf[k, e, r * grp:(r + 1) * grp, n:n + wide] = got[e * grp:(e + 1) * grp, :]

    def shared_hidden(i):
        wait(shared_copies(i, i))
        for n, w in mids:
            vals = []
            for b in range(2):
                v = jnp.dot(hall[0, 0, 0:rows, :], ring[2 * i, b, :, n:n + w], preferred_element_type=F32)
                vals.append(v + jnp.dot(hall[0, 1, 0:rows, :], ring[2 * i + 1, b, :, n:n + w], preferred_element_type=F32))
            actsh[i, :, n:n + w] = (jax.nn.silu(vals[0]) * vals[1]).astype(BF16)
        for k in range(2):
            start(half_copies(2 * i + k))

    for r in range(4):
        tables(r)
    ga.turn()
    gb.send()
    shared_hidden(0)
    ga.share()
    ga.mate.wait_recv()
    gather_rows(0, 0)
    shared_hidden(1)
    ga.last()
    ga.m_x.wait_recv()
    gather_rows(1, 0)
    ga.m_y.wait_recv()
    gather_rows(2, 0)
    ga.m_da.wait_recv()
    ga.m_db.wait_recv()
    gather_rows(3, 0)

    @pl.loop(0, n_exp)
    def _(e):
        slot = e % 4
        wait(half_copies(e))
        for n, w in mids:
            part[e, :, n:n + w] = jnp.dot(xbuf[0, e], ring[slot, 0, :, n:n + w], preferred_element_type=F32)
            part[e, :, ff + n:ff + n + w] = jnp.dot(xbuf[0, e], ring[slot, 1, :, n:n + w], preferred_element_type=F32)
        start(half_copies(e + 4))

        @pl.when(e == 0)
        def _():
            gb.turn()
            gb.mate.wait_recv()
            gather_rows(0, 1)

        @pl.when(e == 2)
        def _():
            gb.share()

        @pl.when(e == 3)
        def _():
            gb.m_x.wait_recv()
            gather_rows(1, 1)
            gb.m_y.wait_recv()
            gather_rows(2, 1)

        pl.when(e == 4)(gb.last)

        @pl.when(e == 5)
        def _():
            gb.m_da.wait_recv()
            gb.m_db.wait_recv()
            gather_rows(3, 1)

    @pl.loop(0, n_exp)
    def _(e):
        slot = e % 4
        wait(half_copies(n_exp + e))
        late = []
        for n, w in mids:
            g = part[e, :, n:n + w] + jnp.dot(xbuf[1, e], ring[slot, 0, :, n:n + w], preferred_element_type=F32)
            u = part[e, :, ff + n:ff + n + w] + jnp.dot(xbuf[1, e], ring[slot, 1, :, n:n + w], preferred_element_type=F32)
            act = (jax.nn.silu(g) * u).astype(BF16)
            if n < deep:
                xbuf[0, e, :, n:n + w] = act
            else:
                late.append((n - deep, w, act))
        for n, w, act in late:
            xbuf[1, e, :, n:n + w] = act
        pl.when(e < 4)(lambda: start(half_copies(n_exp + e + 4)))
        pl.when(e == 5)(lambda: start(down_copies(0)))
        pl.when(e == 7)(lambda: start(down_copies(1)))

    def acc(j, f, r):
        return part.at[j, pl.ds(0, rows), pl.ds((4 * f + r) * side, side)]

    def base(j, f):
        return part.at[j, pl.ds(0, rows), pl.ds((8 + f) * side, side)]

    def first_stage(j):
        out = []
        for f, dev in enumerate((xn, yn)):
            for q, r in enumerate((1 + f, 3)):
                out.append(remote(acc(j, f, r), r1.at[j, f, q], s1_s.at[j, 2 * f + q], s1_r.at[j, 2 * f + q], dev))
        return out

    def second_stage(j):
        return [remote(acc(j, f, 2 - f), r2.at[j, f], s2_s.at[j, f], s2_r.at[j, f], dev) for f, dev in enumerate((yn, xn))]

    def swap(j):
        return remote(stage.at[j % 2], drecv.at[j], d_s.at[j], d_r.at[j], mate)

    def send_sum(j):
        swap(j).wait_recv()
        for f in range(2):
            for r in range(4):
                acc(j, f, r)[...] = acc(j, f, r)[...] + drecv[j, f, r]
        start(first_stage(j))

    def pass_on(j):
        for c in first_stage(j):
            c.wait_recv()
        for f, c in enumerate(second_stage(j)):
            acc(j, f, 2 - f)[...] = acc(j, f, 2 - f)[...] + r1[j, f, 1]
            c.start()
        for f in range(2):
            acc(j, f, 0)[...] = acc(j, f, 0)[...] + r1[j, f, 0]

    @pl.loop(0, n_chunk)
    def _(j):
        q = j % 2
        wait(down_copies(j))
        for e in range(n_exp):
            head, tail = down_tiles(q, e)
            got = jnp.dot(xbuf[0, e], head[...], preferred_element_type=F32)
            got = (got + jnp.dot(xbuf[1, e, :, 0:left], tail[...], preferred_element_type=F32)).astype(BF16)
            for r in range(4):
                pbuf[r, e * grp:(e + 1) * grp, :] = got[r * grp:(r + 1) * grp, :]
        pl.when(j >= 1)(lambda: send_sum(j - 1))
        pl.when(j >= 2)(lambda: swap(j - 2).wait_send())
        for r in range(4):
            out = jnp.dot(pw[r, 0], pbuf[r], preferred_element_type=F32)
            out = out + jnp.dot(pw[r, 1], pbuf[r], preferred_element_type=F32)
            out = out + jnp.dot(pw[r, 2], pbuf[r], preferred_element_type=F32)
            for f in range(2):
                cut = slice(f * side, (f + 1) * side)
                acc(j, f, r)[...] = out[0:rows, cut]
                stage[q, f, r] = out[rows:, cut]
        swap(j).start()
        pl.when(j + 2 < n_chunk)(lambda: start(down_copies(j + 2)))
        pl.when(j == n_chunk - 2)(lambda: start(shared_down_copies(0)))
        pl.when(j == n_chunk - 1)(lambda: start(shared_down_copies(1)))
        pl.when(j >= LAG)(lambda: pass_on(j - LAG))

    send_sum(n_chunk - 1)


    res_copy.wait()

    @pl.loop(0, 2)
    def _(t):
        wait(shared_down_copies(t))
        for c in range(4):
            j = 4 * t + c
            cols = pl.ds(pl.multiple_of(j * CHUNK, CHUNK), CHUNK)
            total = out_ref[:, cols].astype(F32)
            for i in range(2):
                head, tail = shared_tiles(t, c, i)
                total = total + jnp.dot(actsh[i, :, 0:deep], head[...], preferred_element_type=F32)
                total = total + jnp.dot(actsh[i, :, deep:ff], tail[...], preferred_element_type=F32)
            for f in range(2):
                base(j, f)[...] = total[:, f * side:(f + 1) * side]
        pass_on(n_chunk - 2 + t)

    @pl.loop(0, n_chunk)
    def _(j):
        for f, c in enumerate(second_stage(j)):
            c.wait_recv()
            cols = pl.ds(pl.multiple_of(j * CHUNK + f * side, side), side)
            out_ref[:, cols] = (base(j, f)[...] + (acc(j, f, 0)[...] + r2[j, f])).astype(BF16)

    for c in rw_copies + ga.sends() + gb.sends():
        c.wait_send()
    swap(n_chunk - 2).wait_send()
    swap(n_chunk - 1).wait_send()

    @pl.loop(0, n_chunk)
    def _(j):
        for c in first_stage(j) + second_stage(j):
            c.wait_send()


def moe(h, table, resid, eg, eu, ed, sg, su, sd):
    _, rows, deep = h.shape
    d_model = 2 * deep
    n_exp, _, ff = eg.shape
    n_chunk = d_model // CHUNK
    side = CHUNK // 2
    slots = 8 * CAP
    pairs = 2 * CAP * n_exp
    vmem = pl.BlockSpec(memory_space=pltpu.VMEM)
    hbm = pl.BlockSpec(memory_space=pl.ANY)
    dma = pltpu.SemaphoreType.DMA
    scratch = [
        pltpu.VMEM((4, 2, deep, ff), BF16),
        pltpu.VMEM((4, 2, 2 * rows, deep), BF16),
        pltpu.VMEM((2, n_exp, slots, deep), BF16),
        pltpu.VMEM((n_exp, slots, 2 * ff), F32),
        pltpu.VMEM((2, rows, ff), BF16),
        pltpu.VMEM((n_chunk, 2, 4, rows, side), F32),
        pltpu.VMEM((n_chunk, 2, 2, rows, side), F32),
        pltpu.VMEM((n_chunk, 2, rows, side), F32),
        pltpu.VMEM((2, 2, 4, rows, side), F32),
        pltpu.VMEM((4, 3, 2 * rows, pairs), BF16),
        pltpu.VMEM((pairs, 2 * rows), F32),
        pltpu.VMEM((4, pairs, 2 * rows), BF16),
        pltpu.VMEM((4, 2, n_exp, rows), F32),
        pltpu.VMEM(table.shape, F32),
        dma((4, 8)), dma((4,)), dma((2, 11)), dma((2, 11)), dma((7,)), dma((7,)), dma((n_chunk,)), dma((n_chunk,)),
        dma((n_chunk, 4)), dma((n_chunk, 4)), dma((n_chunk, 2)), dma((n_chunk, 2)),
    ]
    return pl.pallas_call(
        moe_kernel,
        out_shape=jax.ShapeDtypeStruct((rows, d_model), BF16),
        in_specs=[hbm] * 9,
        out_specs=vmem,
        scratch_shapes=scratch,
        compiler_params=pltpu.CompilerParams(collective_id=0, has_side_effects=True, vmem_limit_bytes=67043328),
        cost_estimate=pl.CostEstimate(flops=40_000_000_000, bytes_accessed=175_000_000, transcendentals=0),
    )(h, table, resid, eg, eu, ed, sg, su, sd)


def solution(mesh):
    row_one = P(('dp', 'ep'))
    row_two = P(('dp', 'ep'), None)
    row_three = P(('dp', 'ep'), None, None)
    rep_one = P(None)
    rep_two = P(None, None)
    rep_three = P(None, None, None)
    exp_spec = P('ep', None, None)

    def local_step(tok_in, lat_cache, rope_cache, tok_pos, expert_ids, attn_gain, w_query, w_kvdown, w_ukey, w_uval, w_out, ffn_gain, w_router, sh_gate, sh_up, sh_down, ex_gate, ex_up, ex_down):
        resid_bf, h_norm, table, lat_out, rope_out = attention(tok_in, lat_cache, rope_cache, tok_pos, expert_ids, attn_gain, w_query, w_kvdown, w_ukey, w_uval, w_out, ffn_gain, w_router)
        out_hidden = moe(h_norm, table, resid_bf, ex_gate, ex_up, ex_down, sh_gate, sh_up, sh_down)
        return out_hidden, lat_out, rope_out

    in_specs = (row_two, row_three, row_three, row_one, row_two, rep_one, rep_two, rep_two, rep_three, rep_three, rep_two, rep_one, rep_two, rep_two, rep_two, rep_two, exp_spec, exp_spec, exp_spec)
    out_specs = (row_two, row_three, row_three)
    return jax.shard_map(local_step, mesh=mesh, in_specs=in_specs, out_specs=out_specs, check_vma=False)
```

```python
import jax
import jax.numpy as jnp
import numpy as np
from jax import lax
from jax.experimental import pallas as pl
from jax.experimental.pallas import tpu as pltpu
from jax.sharding import PartitionSpec as P

ROUTE_SCALE = 2.827
ROPE_BASE = 10000.0
NORM_EPS = 1e-6
CAP = 24
CHUNK = 256
BLK = 16
LAG = 2
F32 = jnp.float32
BF16 = jnp.bfloat16


def attn_kernel(pos_ref, prow_ref, x_ref, gain_ref, ids_ref, fgain_ref, wkv, wq, wuk, wuv, wo, wr, lat_in, rope_in,
                lat_out, rope_out, res_ref, h_ref, rw_ref,
                vkv, vq, vuk, vuv, vo, vr, lat, rop, xn, qlat, qrope, latn, ropen, olat, ohd, w_sem, lat_sem, rope_sem, lo_sem, ro_sem):
    rows, d_model = x_ref.shape
    n_head, nope, rank = wuk.shape
    rdim = rope_in.shape[1]
    seq = lat_in.shape[1]
    qk = nope + rdim
    n_blk = rows // BLK
    scale = qk ** -0.5
    pair = 2 * qk
    n_pair = n_head // 2
    deep = d_model // 2

    def q_copy(m):
        cols = slice(m * pair, (m + 1) * pair)
        return pltpu.make_async_copy(wq.at[:, cols], vq.at[:, cols], w_sem.at[m])

    kv_copy = pltpu.make_async_copy(wkv, vkv, w_sem.at[n_pair])
    uk_copy = pltpu.make_async_copy(wuk, vuk, w_sem.at[n_pair + 1])
    uv_copy = pltpu.make_async_copy(wuv, vuv, w_sem.at[n_pair + 2])
    o_copy = pltpu.make_async_copy(wo, vo, w_sem.at[n_pair + 3])
    r_copy = pltpu.make_async_copy(wr, vr, w_sem.at[n_pair + 4])

    def lat_load(b):
        return pltpu.make_async_copy(lat_in.at[pl.ds(b * BLK, BLK)], lat.at[pl.ds(b * BLK, BLK)], lat_sem.at[b])

    def rope_load(b):
        return pltpu.make_async_copy(rope_in.at[pl.ds(b * BLK, BLK)], rop.at[pl.ds(b * BLK, BLK)], rope_sem.at[b])

    def lat_save(b):
        return pltpu.make_async_copy(lat.at[pl.ds(b * BLK, BLK)], lat_out.at[pl.ds(b * BLK, BLK)], lo_sem.at[b])

    def rope_save(b):
        return pltpu.make_async_copy(rop.at[pl.ds(b * BLK, BLK)], rope_out.at[pl.ds(b * BLK, BLK)], ro_sem.at[b])

    kv_copy.start()
    for m in range(n_pair):
        q_copy(m).start()
        if m == 0:
            uk_copy.start()

    @pl.loop(0, n_blk)
    def _(b):
        lat_load(b).start()
        rope_load(b).start()

    uv_copy.start()
    o_copy.start()
    r_copy.start()

    xw = x_ref[...].astype(F32)
    xn[...] = (xw * lax.rsqrt(jnp.mean(xw * xw, axis=-1, keepdims=True) + NORM_EPS) * gain_ref[...].reshape(1, d_model).astype(F32)).astype(BF16)
    lane = lax.broadcasted_iota(jnp.int32, (rows, 2 * rdim), 1)
    front = lane % rdim < rdim // 2
    low = lane < rdim
    where_in = lane % (rdim // 2)
    freq = jnp.zeros(lane.shape, F32)
    for i in range(rdim // 2):
        freq = jnp.where(where_in == i, np.float32(ROPE_BASE ** (-2.0 * i / rdim)), freq)
    angle = jnp.transpose(jnp.broadcast_to(prow_ref[...].astype(F32), (rows, rows))) * freq
    cos_t = jnp.cos(angle)
    sin_t = jnp.where(front, -jnp.sin(angle), jnp.sin(angle))

    def rotate(v):
        swapped = jnp.where(front, pltpu.roll(v, 2 * rdim - rdim // 2, 1), pltpu.roll(v, rdim // 2, 1))
        return v * cos_t + swapped * sin_t

    kv_copy.wait()
    kv = lax.dot_general(xn[...], vkv[...], (((1,), (1,)), ((), ())), preferred_element_type=F32)
    lat_raw = kv[:, 0:rank]
    latn[...] = (lat_raw * lax.rsqrt(jnp.mean(lat_raw * lat_raw, axis=-1, keepdims=True) + NORM_EPS)).astype(BF16).astype(F32)
    kr = kv[:, rank:rank + rdim]
    ropen[...] = rotate(jnp.concatenate([kr, kr], axis=1)).astype(BF16).astype(F32)

    for m in range(n_pair):
        q_copy(m).wait()
        if m == 0:
            uk_copy.wait()
        qf = jnp.dot(xn[...], vq[:, m * pair:(m + 1) * pair], preferred_element_type=F32).astype(BF16).astype(F32)
        qa, qb, qc = qf[:, 0:nope], qf[:, nope:2 * nope], qf[:, 2 * nope:3 * nope]
        second = pltpu.roll(jnp.where(low, qc, qb), rdim, 1)
        turned = rotate(jnp.where(low, qb, qc))
        qrope[2 * m] = turned[:, 0:rdim].astype(BF16)
        qrope[2 * m + 1] = pltpu.roll(turned, rdim, 1)[:, 0:rdim].astype(BF16)
        qlat[2 * m] = jnp.dot(qa.astype(BF16), vuk[2 * m], preferred_element_type=F32).astype(BF16)
        qlat[2 * m + 1] = jnp.dot(second.astype(BF16), vuk[2 * m + 1], preferred_element_type=F32).astype(BF16)

    grp = BLK * n_head
    row_i = lax.broadcasted_iota(jnp.int32, (grp, grp), 0)
    col_i = lax.broadcasted_iota(jnp.int32, (grp, grp), 1)
    perm = jnp.where(col_i == (row_i % n_head) * BLK + row_i // n_head, 1.0, 0.0).astype(BF16)

    @pl.loop(0, n_blk)
    def _(b):
        t0 = pl.multiple_of(b * BLK, BLK)
        lat_load(b).wait()
        rope_load(b).wait()
        news = jnp.transpose(ropen[pl.ds(t0, BLK), :])
        slane = lax.broadcasted_iota(jnp.int32, (rdim, seq), 1)
        srow = lax.broadcasted_iota(jnp.int32, (16, rank), 0)
        for t in range(BLK):
            p = pos_ref[t0 + t]
            lo = pl.multiple_of((p // 16) * 16, 16)
            old = lat[t0 + t, pl.ds(lo, 16), :]
            lat[t0 + t, pl.ds(lo, 16), :] = jnp.where(srow == p - lo, latn[pl.ds(t0 + t, 1), :], old.astype(F32)).astype(BF16)
            rop[t0 + t] = jnp.where(slane == p, news[0:rdim, t:t + 1], rop[t0 + t].astype(F32)).astype(BF16)
        q_blk = jnp.dot(perm, qlat[:, pl.ds(t0, BLK), :].reshape(grp, rank), preferred_element_type=F32).astype(BF16)
        r_blk = jnp.dot(perm, qrope[:, pl.ds(t0, BLK), :].reshape(grp, rdim), preferred_element_type=F32).astype(BF16)
        klane = lax.broadcasted_iota(jnp.int32, (n_head, seq), 1)
        scores = []
        for t in range(BLK):
            s = lax.dot_general(q_blk[t * n_head:(t + 1) * n_head], lat[t0 + t], (((1,), (1,)), ((), ())), preferred_element_type=F32)
            s = s + jnp.dot(r_blk[t * n_head:(t + 1) * n_head], rop[t0 + t], preferred_element_type=F32)
            scores.append(jnp.where(klane <= pos_ref[t0 + t], s * scale, -jnp.inf))
        sc = jnp.concatenate(scores, axis=0)
        ex = jnp.exp(sc - jnp.max(sc, axis=-1, keepdims=True))
        prob = (ex / jnp.sum(ex, axis=-1, keepdims=True)).astype(BF16)
        outs = [jnp.dot(prob[t * n_head:(t + 1) * n_head], lat[t0 + t], preferred_element_type=F32).astype(BF16) for t in range(BLK)]
        mixed = jnp.dot(perm, jnp.concatenate(outs, axis=0), preferred_element_type=F32).astype(BF16)
        olat[:, pl.ds(t0, BLK), :] = mixed.reshape(n_head, BLK, rank)
        lat_save(b).start()
        rope_save(b).start()

    uv_copy.wait()
    for h in range(n_head):
        ohd[:, h * nope:(h + 1) * nope] = jnp.dot(olat[h], vuv[h], preferred_element_type=F32).astype(BF16)
    o_copy.wait()
    total = jnp.zeros((rows, 1), F32)
    wide = 512
    for n in range(0, d_model, wide):
        part = jnp.dot(ohd[...], vo[:, n:n + wide], preferred_element_type=F32)
        res = (x_ref[:, n:n + wide].astype(F32) + part).astype(BF16)
        res_ref[:, n:n + wide] = res
        resf = res.astype(F32)
        total = total + jnp.sum(resf * resf, axis=-1, keepdims=True)
    fgain = fgain_ref[...].reshape(1, d_model).astype(F32)
    inv = lax.rsqrt(total * (1.0 / d_model) + NORM_EPS)
    for n in range(0, d_model, wide):
        h_ref[n // deep, :, n % deep:n % deep + wide] = (res_ref[:, n:n + wide].astype(F32) * inv * fgain[:, n:n + wide]).astype(BF16)
    r_copy.wait()
    logits = [lax.dot_general(vr[:, k * deep:(k + 1) * deep], h_ref[k], (((1,), (1,)), ((), ())), preferred_element_type=F32) for k in range(2)]
    gate = jax.nn.sigmoid(logits[0] + logits[1])
    want = lax.broadcasted_iota(jnp.int32, gate.shape, 0)
    picked = want == ids_ref[0:1, :]
    for k in range(1, ids_ref.shape[0]):
        picked = picked | (want == ids_ref[k:k + 1, :])
    chosen = jnp.where(picked, gate, 0.0)
    rw_ref[...] = ROUTE_SCALE * chosen / jnp.sum(chosen, axis=0, keepdims=True)

    @pl.loop(0, n_blk)
    def _(b):
        lat_save(b).wait()
        rope_save(b).wait()


def attention(tok_in, lat_cache, rope_cache, tok_pos, expert_ids, attn_gain, w_query, w_kvdown, w_ukey, w_uval, w_out, ffn_gain, w_router):
    rows, d_model = tok_in.shape
    n_head, nope, rank = w_ukey.shape
    seq, rdim = rope_cache.shape[1], rope_cache.shape[2]
    n_exp = w_router.shape[1]
    vmem = pl.BlockSpec(memory_space=pltpu.VMEM)
    smem = pl.BlockSpec(memory_space=pltpu.SMEM)
    hbm = pl.BlockSpec(memory_space=pl.ANY)
    dma = pltpu.SemaphoreType.DMA
    n_blk = rows // BLK
    scratch = [
        pltpu.VMEM((rank + rdim, d_model), BF16),
        pltpu.VMEM(w_query.shape, BF16),
        pltpu.VMEM(w_ukey.shape, BF16),
        pltpu.VMEM(w_uval.shape, BF16),
        pltpu.VMEM(w_out.shape, BF16),
        pltpu.VMEM((n_exp, d_model), BF16),
        pltpu.VMEM(lat_cache.shape, BF16),
        pltpu.VMEM((rows, rdim, seq), BF16),
        pltpu.VMEM((rows, d_model), BF16),
        pltpu.VMEM((n_head, rows, rank), BF16),
        pltpu.VMEM((n_head, rows, rdim), BF16),
        pltpu.VMEM((rows, rank), F32),
        pltpu.VMEM((rows, 2 * rdim), F32),
        pltpu.VMEM((n_head, rows, rank), BF16),
        pltpu.VMEM((rows, n_head * nope), BF16),
        dma((n_head // 2 + 5,)), dma((n_blk,)), dma((n_blk,)), dma((n_blk,)), dma((n_blk,)),
    ]
    lat_out, rope_out, resid, h, table = pl.pallas_call(
        attn_kernel,
        out_shape=(
            jax.ShapeDtypeStruct(lat_cache.shape, BF16),
            jax.ShapeDtypeStruct((rows, rdim, seq), BF16),
            jax.ShapeDtypeStruct((rows, d_model), BF16),
            jax.ShapeDtypeStruct((2, rows, d_model // 2), BF16),
            jax.ShapeDtypeStruct((n_exp, rows), F32),
        ),
        in_specs=[smem] + [vmem] * 5 + [hbm] * 8,
        out_specs=(hbm, hbm, vmem, vmem, vmem),
        scratch_shapes=scratch,
        compiler_params=pltpu.CompilerParams(vmem_limit_bytes=64000000),
        cost_estimate=pl.CostEstimate(flops=5_000_000_000, bytes_accessed=66_000_000, transcendentals=0),
    )(tok_pos, tok_pos[None, :], tok_in, attn_gain, expert_ids.T, ffn_gain,
      w_kvdown.T, w_query, w_ukey, w_uval, w_out, w_router.T, lat_cache, jnp.swapaxes(rope_cache, 1, 2))
    return resid, h, table, lat_out, jnp.swapaxes(rope_out, 1, 2)


def moe_kernel(h_hbm, rw_hbm, res_hbm, eg, eu, ed, sg, su, sd, out_hbm,
               ring, hall, xbuf, part, actsh, drecv, r1, r2, stage, pw, pwf, pbuf, rwin, rw_ref, out_ref,
               ring_sem, in_sem, out_sem, ag_s, ag_r, rw_s, rw_r, d_s, d_r, s1_s, s1_r, s2_s, s2_r):
    rows = rw_hbm.shape[1]
    half = rows // 2
    deep = h_hbm.shape[2]
    d_model = 2 * deep
    ff = eg.shape[2]
    n_exp = eg.shape[0]
    n_chunk = d_model // CHUNK
    side = CHUNK // 2
    grp = 2 * CAP
    left = ff - deep
    mids = [(n, min(CHUNK, ff - n)) for n in range(0, ff, CHUNK)]
    me = lax.axis_index('ep')
    core = me % 2
    cx = (me // 2) % 2
    cy = me // 4
    mate = me + 1 - 2 * core
    xn = me + 2 - 4 * cx
    yn = me + 4 - 8 * cy
    dg = yn + 2 - 4 * cx
    others = [(0, 1, mate), (1, 0, xn), (1, 1, xn + 1 - 2 * core), (2, 0, yn), (2, 1, yn + 1 - 2 * core), (3, 0, dg), (3, 1, dg + 1 - 2 * core)]

    def remote(src, dst, ssem, rsem, dev):
        return pltpu.make_async_remote_copy(src_ref=src, dst_ref=dst, send_sem=ssem, recv_sem=rsem, device_id={'ep': dev}, device_id_type=pl.DeviceIdType.MESH)

    def start(copies):
        for c in copies:
            c.start()

    def wait(copies):
        for c in copies:
            c.wait()

    step = deep // 2

    def block_copies(slot, gate, up, k, col):
        out = []
        for b, src in enumerate((gate, up)):
            for q in range(2):
                at = pl.ds(pl.multiple_of(k * deep + q * step, step), step)
                out.append(pltpu.make_async_copy(src.at[at, col], ring.at[slot, b, pl.ds(q * step, step), :], ring_sem.at[slot, 2 * b + q]))
        return out

    def half_copies(i):
        e = i % n_exp
        return block_copies(i % 4, eg.at[e], eu.at[e], i // n_exp, slice(None))

    def shared_copies(q, i):
        col = pl.ds(pl.multiple_of(i * ff, side), ff)
        return block_copies(2 * q, sg, su, 0, col) + block_copies(2 * q + 1, sg, su, 1, col)

    def tile(q, g, lo, size):
        return ring.at[2 * q + g // 10, (g // 5) % 2, pl.ds(lo, size), pl.ds((g % 5) * CHUNK, CHUNK)]

    def pair_sem(q, i):
        return ring_sem.at[2 * q + i // 8, i % 8]

    def down_tiles(q, e):
        return tile(q, e, 0, deep), tile(q, n_exp + e // 2, (e % 2) * left, left)

    def down_copies(j):
        q = j % 2
        cols = pl.ds(pl.multiple_of(j * CHUNK, CHUNK), CHUNK)
        out = []
        for e in range(n_exp):
            head, tail = down_tiles(q, e)
            out.append(pltpu.make_async_copy(ed.at[e, pl.ds(0, deep), cols], head, pair_sem(q, 2 * e)))
            out.append(pltpu.make_async_copy(ed.at[e, pl.ds(deep, left), cols], tail, pair_sem(q, 2 * e + 1)))
        return out

    def shared_tiles(q, c, i):
        return tile(q, 3 * c + i, 0, deep), tile(q, 3 * c + 2, i * left, left)

    def shared_down_copies(t):
        out = []
        for c in range(4):
            cols = pl.ds(pl.multiple_of((4 * t + c) * CHUNK, CHUNK), CHUNK)
            for i in range(2):
                head, tail = shared_tiles(t, c, i)
                out.append(pltpu.make_async_copy(sd.at[pl.ds(i * ff, deep), cols], head, pair_sem(t, 4 * c + 2 * i)))
                out.append(pltpu.make_async_copy(sd.at[pl.ds(i * ff + deep, left), cols], tail, pair_sem(t, 4 * c + 2 * i + 1)))
        return out

    barrier = pltpu.get_barrier_semaphore()
    for _, _, dev in others:
        pl.semaphore_signal(barrier, inc=1, device_id={'ep': dev}, device_id_type=pl.DeviceIdType.MESH)
    in_copies = [pltpu.make_async_copy(h_hbm.at[k], hall.at[0, k, pl.ds(0, rows)], in_sem.at[k]) for k in range(2)]
    in_copies.append(pltpu.make_async_copy(rw_hbm, rw_ref, in_sem.at[2]))
    res_copy = pltpu.make_async_copy(res_hbm, out_ref, in_sem.at[3])
    start(in_copies)
    wait(in_copies)
    start(shared_copies(0, 0))
    start(shared_copies(1, 1))
    res_copy.start()
    pl.semaphore_wait(barrier, len(others))

    part_a, part_b = pl.ds(0, half), pl.ds(half, half)
    own, other = pl.ds(0, rows), pl.ds(rows, rows)
    rw_copies = [remote(rw_ref.at[pl.ds(pl.multiple_of(dev * n_exp, n_exp), n_exp), :], rwin.at[r, p], rw_s.at[i], rw_r.at[i], dev) for i, (r, p, dev) in enumerate(others)]

    class Gather:
        def __init__(self, k):
            def hop(i, src, dst, dev):
                return remote(src, dst, ag_s.at[k, i], ag_r.at[k, i], dev)
            self.mate = hop(0, hall.at[0, k, own], hall.at[0, k, other], mate)
            self.x_a = hop(1, hall.at[0, k, part_a], hall.at[1, k, part_a], xn)
            self.x_b = hop(2, hall.at[0, k, part_b], hall.at[1, k, part_b], xn)
            self.y_b = hop(3, hall.at[0, k, part_b], hall.at[2, k, part_b], yn)
            self.y_a = hop(4, hall.at[0, k, part_a], hall.at[2, k, part_a], yn)
            self.d_a = hop(5, hall.at[1, k, part_a], hall.at[3, k, part_a], yn)
            self.d_b = hop(6, hall.at[2, k, part_b], hall.at[3, k, part_b], xn)
            self.m_x = hop(7, hall.at[1, k, own], hall.at[1, k, other], mate)
            self.m_y = hop(8, hall.at[2, k, own], hall.at[2, k, other], mate)
            self.m_da = hop(9, hall.at[3, k, part_a], hall.at[3, k, pl.ds(rows, half)], mate)
            self.m_db = hop(10, hall.at[3, k, part_b], hall.at[3, k, pl.ds(rows + half, half)], mate)

        def send(self):
            start([self.x_a, self.y_b, self.x_b, self.y_a, self.mate])

        def turn(self):
            self.x_a.wait_recv()
            self.d_a.start()
            self.y_b.wait_recv()
            self.d_b.start()

        def share(self):
            self.x_b.wait_recv()
            self.m_x.start()
            self.y_a.wait_recv()
            self.m_y.start()

        def last(self):
            self.d_a.wait_recv()
            self.m_da.start()
            self.d_b.wait_recv()
            self.m_db.start()

        def sends(self):
            return [self.mate, self.x_a, self.x_b, self.y_b, self.y_a, self.d_a, self.d_b, self.m_x, self.m_y, self.m_da, self.m_db]

    ga, gb = Gather(0), Gather(1)
    ga.send()
    start(rw_copies)

    rwin[0, 0] = rw_ref[pl.ds(pl.multiple_of(me * n_exp, n_exp), n_exp), :]
    for c in rw_copies:
        c.wait_recv()

    def tables(r):
        both = jnp.concatenate([rwin[r, 0], rwin[r, 1]], axis=1)
        two = 2 * rows
        t_in = lax.broadcasted_iota(jnp.int32, (two, two), 0)
        t_out = lax.broadcasted_iota(jnp.int32, (two, two), 1)
        ahead = jnp.where((t_in < t_out) & ((t_in < rows) == (t_out < rows)), 1.0, 0.0).astype(BF16)
        picked = both > 0.0
        before = jnp.dot(jnp.where(picked, 1.0, 0.0).astype(BF16), ahead, preferred_element_type=F32)
        lane = lax.broadcasted_iota(jnp.int32, (n_exp, two), 1)
        slot = jnp.where(picked, before + jnp.where(lane < rows, 0.0, float(CAP)), -1.0).astype(jnp.int32)
        want = lax.broadcasted_iota(jnp.int32, (grp, two), 0)
        for e in range(n_exp):
            hit = want == slot[e:e + 1, :]
            pbuf[r, e * grp:(e + 1) * grp, :] = jnp.where(hit, 1.0, 0.0).astype(BF16)
            pwf[e * grp:(e + 1) * grp, :] = jnp.where(hit, both[e:e + 1, :], 0.0)
        turned = pwf[...].T
        hi = turned.astype(BF16)
        rest = turned - hi.astype(F32)
        mid = rest.astype(BF16)
        pw[r, 0] = hi
        pw[r, 1] = mid
        pw[r, 2] = (rest - mid.astype(F32)).astype(BF16)

    def gather_rows(r, k):
        wide = 512
        for n in range(0, deep, wide):
            got = jnp.dot(pbuf[r], hall[r, k, :, n:n + wide], preferred_element_type=F32).astype(BF16)
            for e in range(n_exp):
                xbuf[k, e, r * grp:(r + 1) * grp, n:n + wide] = got[e * grp:(e + 1) * grp, :]

    def shared_hidden(i):
        wait(shared_copies(i, i))
        for n, w in mids:
            vals = []
            for b in range(2):
                v = jnp.dot(hall[0, 0, 0:rows, :], ring[2 * i, b, :, n:n + w], preferred_element_type=F32)
                vals.append(v + jnp.dot(hall[0, 1, 0:rows, :], ring[2 * i + 1, b, :, n:n + w], preferred_element_type=F32))
            actsh[i, :, n:n + w] = (jax.nn.silu(vals[0]) * vals[1]).astype(BF16)
        for k in range(2):
            start(half_copies(2 * i + k))

    for r in range(4):
        tables(r)
    ga.turn()
    gb.send()
    shared_hidden(0)
    ga.share()
    ga.mate.wait_recv()
    gather_rows(0, 0)
    shared_hidden(1)
    ga.last()
    ga.m_x.wait_recv()
    gather_rows(1, 0)
    ga.m_y.wait_recv()
    gather_rows(2, 0)
    ga.m_da.wait_recv()
    ga.m_db.wait_recv()
    gather_rows(3, 0)

    @pl.loop(0, n_exp)
    def _(e):
        slot = e % 4
        wait(half_copies(e))
        for n, w in mids:
            part[e, :, n:n + w] = jnp.dot(xbuf[0, e], ring[slot, 0, :, n:n + w], preferred_element_type=F32)
            part[e, :, ff + n:ff + n + w] = jnp.dot(xbuf[0, e], ring[slot, 1, :, n:n + w], preferred_element_type=F32)
        start(half_copies(e + 4))

        @pl.when(e == 0)
        def _():
            gb.turn()
            gb.mate.wait_recv()
            gather_rows(0, 1)

        @pl.when(e == 2)
        def _():
            gb.share()

        @pl.when(e == 3)
        def _():
            gb.m_x.wait_recv()
            gather_rows(1, 1)
            gb.m_y.wait_recv()
            gather_rows(2, 1)

        pl.when(e == 4)(gb.last)

        @pl.when(e == 5)
        def _():
            gb.m_da.wait_recv()
            gb.m_db.wait_recv()
            gather_rows(3, 1)

    @pl.loop(0, n_exp)
    def _(e):
        slot = e % 4
        wait(half_copies(n_exp + e))
        late = []
        for n, w in mids:
            g = part[e, :, n:n + w] + jnp.dot(xbuf[1, e], ring[slot, 0, :, n:n + w], preferred_element_type=F32)
            u = part[e, :, ff + n:ff + n + w] + jnp.dot(xbuf[1, e], ring[slot, 1, :, n:n + w], preferred_element_type=F32)
            act = (jax.nn.silu(g) * u).astype(BF16)
            if n < deep:
                xbuf[0, e, :, n:n + w] = act
            else:
                late.append((n - deep, w, act))
        for n, w, act in late:
            xbuf[1, e, :, n:n + w] = act
        pl.when(e < 4)(lambda: start(half_copies(n_exp + e + 4)))
        pl.when(e == 5)(lambda: start(down_copies(0)))
        pl.when(e == 7)(lambda: start(down_copies(1)))

    def acc(j, f, r):
        return part.at[j, pl.ds(0, rows), pl.ds((4 * f + r) * side, side)]

    def base(j, f):
        return part.at[j, pl.ds(0, rows), pl.ds((8 + f) * side, side)]

    def first_stage(j):
        out = []
        for f, dev in enumerate((xn, yn)):
            for q, r in enumerate((1 + f, 3)):
                out.append(remote(acc(j, f, r), r1.at[j, f, q], s1_s.at[j, 2 * f + q], s1_r.at[j, 2 * f + q], dev))
        return out

    def second_stage(j):
        return [remote(acc(j, f, 2 - f), r2.at[j, f], s2_s.at[j, f], s2_r.at[j, f], dev) for f, dev in enumerate((yn, xn))]

    def swap(j):
        return remote(stage.at[j % 2], drecv.at[j], d_s.at[j], d_r.at[j], mate)

    def send_sum(j):
        swap(j).wait_recv()
        for f in range(2):
            for r in range(4):
                acc(j, f, r)[...] = acc(j, f, r)[...] + drecv[j, f, r]
        start(first_stage(j))

    def pass_on(j):
        for c in first_stage(j):
            c.wait_recv()
        for f, c in enumerate(second_stage(j)):
            acc(j, f, 2 - f)[...] = acc(j, f, 2 - f)[...] + r1[j, f, 1]
            c.start()
        for f in range(2):
            acc(j, f, 0)[...] = acc(j, f, 0)[...] + r1[j, f, 0]

    @pl.loop(0, n_chunk)
    def _(j):
        q = j % 2
        wait(down_copies(j))
        for e in range(n_exp):
            head, tail = down_tiles(q, e)
            got = jnp.dot(xbuf[0, e], head[...], preferred_element_type=F32)
            got = (got + jnp.dot(xbuf[1, e, :, 0:left], tail[...], preferred_element_type=F32)).astype(BF16)
            for r in range(4):
                pbuf[r, e * grp:(e + 1) * grp, :] = got[r * grp:(r + 1) * grp, :]
        pl.when(j >= 1)(lambda: send_sum(j - 1))
        pl.when(j >= 2)(lambda: swap(j - 2).wait_send())
        for r in range(4):
            out = jnp.dot(pw[r, 0], pbuf[r], preferred_element_type=F32)
            out = out + jnp.dot(pw[r, 1], pbuf[r], preferred_element_type=F32)
            out = out + jnp.dot(pw[r, 2], pbuf[r], preferred_element_type=F32)
            for f in range(2):
                cut = slice(f * side, (f + 1) * side)
                acc(j, f, r)[...] = out[0:rows, cut]
                stage[q, f, r] = out[rows:, cut]
        swap(j).start()
        pl.when(j + 2 < n_chunk)(lambda: start(down_copies(j + 2)))
        pl.when(j == n_chunk - 2)(lambda: start(shared_down_copies(0)))
        pl.when(j == n_chunk - 1)(lambda: start(shared_down_copies(1)))
        pl.when(j >= LAG)(lambda: pass_on(j - LAG))

    send_sum(n_chunk - 1)


    res_copy.wait()

    @pl.loop(0, 2)
    def _(t):
        wait(shared_down_copies(t))
        for c in range(4):
            j = 4 * t + c
            cols = pl.ds(pl.multiple_of(j * CHUNK, CHUNK), CHUNK)
            total = out_ref[:, cols].astype(F32)
            for i in range(2):
                head, tail = shared_tiles(t, c, i)
                total = total + jnp.dot(actsh[i, :, 0:deep], head[...], preferred_element_type=F32)
                total = total + jnp.dot(actsh[i, :, deep:ff], tail[...], preferred_element_type=F32)
            for f in range(2):
                base(j, f)[...] = total[:, f * side:(f + 1) * side]
        pass_on(n_chunk - 2 + t)

    def out_copy(j):
        cols = pl.ds(pl.multiple_of(j * CHUNK, CHUNK), CHUNK)
        return pltpu.make_async_copy(out_ref.at[:, cols], out_hbm.at[:, cols], out_sem.at[j])

    @pl.loop(0, n_chunk)
    def _(j):
        for f, c in enumerate(second_stage(j)):
            c.wait_recv()
            cols = pl.ds(pl.multiple_of(j * CHUNK + f * side, side), side)
            out_ref[:, cols] = (base(j, f)[...] + (acc(j, f, 0)[...] + r2[j, f])).astype(BF16)
        out_copy(j).start()

    for c in rw_copies + ga.sends() + gb.sends():
        c.wait_send()
    swap(n_chunk - 2).wait_send()
    swap(n_chunk - 1).wait_send()

    @pl.loop(0, n_chunk)
    def _(j):
        for c in first_stage(j) + second_stage(j):
            c.wait_send()
        out_copy(j).wait()


def moe(h, table, resid, eg, eu, ed, sg, su, sd):
    _, rows, deep = h.shape
    d_model = 2 * deep
    n_exp, _, ff = eg.shape
    n_chunk = d_model // CHUNK
    side = CHUNK // 2
    slots = 8 * CAP
    pairs = 2 * CAP * n_exp
    hbm = pl.BlockSpec(memory_space=pl.ANY)
    dma = pltpu.SemaphoreType.DMA
    scratch = [
        pltpu.VMEM((4, 2, deep, ff), BF16),
        pltpu.VMEM((4, 2, 2 * rows, deep), BF16),
        pltpu.VMEM((2, n_exp, slots, deep), BF16),
        pltpu.VMEM((n_exp, slots, 2 * ff), F32),
        pltpu.VMEM((2, rows, ff), BF16),
        pltpu.VMEM((n_chunk, 2, 4, rows, side), F32),
        pltpu.VMEM((n_chunk, 2, 2, rows, side), F32),
        pltpu.VMEM((n_chunk, 2, rows, side), F32),
        pltpu.VMEM((2, 2, 4, rows, side), F32),
        pltpu.VMEM((4, 3, 2 * rows, pairs), BF16),
        pltpu.VMEM((pairs, 2 * rows), F32),
        pltpu.VMEM((4, pairs, 2 * rows), BF16),
        pltpu.VMEM((4, 2, n_exp, rows), F32),
        pltpu.VMEM(table.shape, F32),
        pltpu.VMEM((rows, d_model), BF16),
        dma((4, 8)), dma((4,)), dma((n_chunk,)), dma((2, 11)), dma((2, 11)), dma((7,)), dma((7,)), dma((n_chunk,)), dma((n_chunk,)),
        dma((n_chunk, 4)), dma((n_chunk, 4)), dma((n_chunk, 2)), dma((n_chunk, 2)),
    ]
    return pl.pallas_call(
        moe_kernel,
        out_shape=jax.ShapeDtypeStruct((rows, d_model), BF16),
        in_specs=[hbm] * 9,
        out_specs=hbm,
        scratch_shapes=scratch,
        compiler_params=pltpu.CompilerParams(collective_id=0, has_side_effects=True, vmem_limit_bytes=67043328),
        cost_estimate=pl.CostEstimate(flops=40_000_000_000, bytes_accessed=175_000_000, transcendentals=0),
    )(h, table, resid, eg, eu, ed, sg, su, sd)


def solution(mesh):
    row_one = P(('dp', 'ep'))
    row_two = P(('dp', 'ep'), None)
    row_three = P(('dp', 'ep'), None, None)
    rep_one = P(None)
    rep_two = P(None, None)
    rep_three = P(None, None, None)
    exp_spec = P('ep', None, None)

    def local_step(tok_in, lat_cache, rope_cache, tok_pos, expert_ids, attn_gain, w_query, w_kvdown, w_ukey, w_uval, w_out, ffn_gain, w_router, sh_gate, sh_up, sh_down, ex_gate, ex_up, ex_down):
        resid_bf, h_norm, table, lat_out, rope_out = attention(tok_in, lat_cache, rope_cache, tok_pos, expert_ids, attn_gain, w_query, w_kvdown, w_ukey, w_uval, w_out, ffn_gain, w_router)
        out_hidden = moe(h_norm, table, resid_bf, ex_gate, ex_up, ex_down, sh_gate, sh_up, sh_down)
        return out_hidden, lat_out, rope_out

    in_specs = (row_two, row_three, row_three, row_one, row_two, rep_one, rep_two, rep_two, rep_three, rep_three, rep_two, rep_one, rep_two, rep_two, rep_two, rep_two, exp_spec, exp_spec, exp_spec)
    out_specs = (row_two, row_three, row_three)
    return jax.shard_map(local_step, mesh=mesh, in_specs=in_specs, out_specs=out_specs, check_vma=False)
```
